128 devices in a mesh: dp: 8 (over z, core), expert: 16 (over y, x).
Axes of the slice: x: 4, y: 4, z: 4, core: 2. Of those that a mesh axis runs over, the one named last changes fastest.
Arguments:
- frames: bfloat16 [16384, 1024], P(('dp', 'expert')), may hold values from -6 to 6
- norm_gain: float32 [1024], replicated, may hold values from 0.5 to 1.5
- norm_bias: float32 [1024], replicated, may hold values from -3 to 3
- routes: int32 [16384, 2], P(('dp', 'expert')), may hold values from 0 to 31, all different within a row; in each aligned block of 128 rows (0 to 127, 128 to 255, ...) at most 16 rows name the same one
- gate_codes: int32 [16384, 2], P(('dp', 'expert')), may hold values from 1 to 255
- limits: int32 [32], replicated, may hold values from 8 to 16
- up_weight: bfloat16 [128, 1024, 1024], P(('dp', 'expert')), may hold values from -0.1875 to 0.1875
- up_bias: float32 [128, 1024], P(('dp', 'expert')), may hold values from -3 to 3
- down_weight: bfloat16 [128, 1024, 1024], P(('dp', 'expert')), may hold values from -0.09375 to 0.09375
- down_bias: float32 [32, 1024], replicated, may hold values from -2 to 2
Outputs:
- mixed: bfloat16 [16384, 1024], P(('dp', 'expert'))
- load: int32 [32], replicated
The draws below stay inside these ranges and needn't reach their ends.
Inputs may be any that keep to these rules, and one draw needn't show every extreme that they name: `routes`: in each aligned block of 128 rows (the rows of one device) no expert is named by more than 16 rows, and some block has an expert named by exactly 16 rows; the two entries of a row differ.
All inputs are finite; a program needn't handle non-finite values.
Results may differ from the reference program's by a relative error of at most 0.0051.
Values may be sent and summed in bfloat16 or wider, within the bound.
A program may use at most 64 MiB of HBM per device.

```python
import math
import jax
import jax.numpy as jnp
import numpy as np
from jax import lax

D = 1024
FF = 4096
TOK_DEV = 128
EXPERTS = 32
SHARDS = 4
FF_DEV = 1024
CAP = 16
TOKENS = 16384
N_DP = 8
N_EXPERT = 16


def plant(array, rng, least, high):
    longest = array.shape.index(max(array.shape))
    spots = []
    for shift in (0, 1):
        where = [jax.random.randint(jax.random.fold_in(rng, axis), (), 0, length) for axis, length in enumerate(array.shape)]
        where[longest] = (where[longest] + shift) % array.shape[longest]
        spots.append(tuple(where))
    return array.at[spots[0]].set(least).at[spots[1]].set(high)


def level_of(own_key, shape, pieces, low, top_value):
    def one(axis_at, shards_of):
        heights = jax.random.uniform(jax.random.fold_in(jax.random.fold_in(own_key, 6), axis_at), (shards_of,), jnp.float32, low / len(pieces), top_value / len(pieces))
        return jnp.repeat(jnp.exp(heights), shape[axis_at] // shards_of).reshape((-1,) + (1,) * (len(shape) - axis_at - 1))

    gain = one(*pieces[0])
    for cut in pieces[1:]:
        gain = gain * one(*cut)
    return gain


def shared_out(key, own, number, rows, number_of, top, limit, skew):
    sequence = jax.random.permutation(key, number_of)
    packed, usual = load_shares(number_of, rows * top, limit, skew, True), load_shares(number_of, rows * top, limit, skew, False)
    places = jnp.arange(number_of)

    def named(lengths, turn):
        used = int((lengths > 0).sum())
        fixed = max(1, used // 4)
        moved = fixed + (places - fixed + turn * (used - fixed)) % max(1, number_of - fixed)
        return jnp.zeros((number_of,), jnp.int32).at[sequence[jnp.where(places < fixed, places, moved)]].set(jnp.asarray(lengths, jnp.int32))

    lengths = jnp.where(number % 4 == 0, named(packed, number // 4), named(usual, number - number // 4 - 1))
    mixed = jax.random.permutation(jax.random.fold_in(own, 3), number_of)
    giver, receiver = mixed[0:number_of // 2 * 2:2], mixed[1:number_of // 2 * 2:2]
    room = jnp.minimum(lengths[giver] - 1, limit - lengths[receiver]) // 2
    room = jnp.where((giver == sequence[0]) | (receiver == sequence[0]) | (lengths[receiver] == 0), 0, jnp.maximum(room, 0))
    moved = jax.random.randint(jax.random.fold_in(own, 4), (number_of // 2,), 0, 1 << 20) % (room + 1)
    lengths = lengths.at[giver].add(-moved).at[receiver].add(moved)
    members = jnp.searchsorted(jnp.cumsum(lengths), jnp.arange(rows * top), side="right").astype(jnp.int32)
    table = members.reshape(top, rows).T
    table = table[jax.random.permutation(jax.random.fold_in(own, 1), rows)]
    turn = jax.random.randint(jax.random.fold_in(own, 2), (rows, 1), 0, top)
    return jnp.take_along_axis(table, (jnp.arange(top)[None, :] + turn) % top, axis=1)


def load_shares(count, total, reach, lean, full):
    portions = [(1 << 20) // math.isqrt(grade ** lean) + 1 for grade in range(1, count + 1)]
    largest = reach if full else min(reach, max(-(-total // count), total * portions[0] // sum(portions)))
    least = 1 if total - largest >= count - 1 else 0
    holding, rest = [largest] + [least] * (count - 1), total - largest - least * (count - 1)
    while rest > 0:
        candidates = [i for i in range(1, count) if holding[i] < largest] or [i for i in range(1, count) if holding[i] < reach]
        whole, left = sum([portions[i] for i in candidates]), rest
        for i in candidates:
            extra = min(reach - holding[i], max(1, left * portions[i] // whole), rest)
            holding[i] = holding[i] + extra
            rest = rest - extra
    return np.array(holding)


def gaussian(stream_key, dims, scale, bound, shards=(), held_as=jnp.bfloat16):
    values = scale * jax.random.normal(stream_key, dims, jnp.float32)
    if shards:
        values = values * level_of(stream_key, dims, shards, -0.22, 0.18)
    return jnp.clip(values, -bound, bound).astype(held_as)


def setup_inputs(seed: int = 0) -> dict:
    keys = jax.random.split(jax.random.key(seed), 11)
    frames = gaussian(keys[0], (TOKENS, D), 1.0, 6.0, ((0, 128),))
    norm_gain = jnp.clip(jax.random.uniform(keys[1], (D,), jnp.float32, 0.5, 1.5), 0.5, 1.5)
    norm_bias = gaussian(keys[2], (D,), 0.5, 3.0, (), jnp.float32)
    routes_keys = jax.random.split(jax.random.fold_in(keys[3], 1), TOKENS // TOK_DEV)
    routes_turns = jax.random.permutation(jax.random.fold_in(keys[3], 3), TOKENS // TOK_DEV)
    routes = jax.vmap(lambda own, number: shared_out(jax.random.fold_in(keys[3], 2), own, number, TOK_DEV, EXPERTS, 2, CAP, 2))(routes_keys, routes_turns).reshape((TOKENS, 2))
    gate_codes = plant(jax.random.randint(keys[4], (TOKENS, 2), 1, 256), jax.random.fold_in(keys[4], 1), 1, 255).astype(jnp.int32)
    limits = plant(jax.random.randint(keys[5], (EXPERTS,), CAP // 2, CAP + 1), jax.random.fold_in(keys[5], 1), CAP // 2, CAP).astype(jnp.int32)
    up_weight = gaussian(keys[6], (EXPERTS * SHARDS, D, FF_DEV), D ** -0.5, 0.1875, ((0, 128),))
    up_bias = gaussian(keys[7], (EXPERTS * SHARDS, FF_DEV), 0.5, 3.0, ((0, 128),), jnp.float32)
    down_weight = gaussian(keys[8], (EXPERTS * SHARDS, FF_DEV, D), FF ** -0.5, 0.09375, ((0, 128),))
    down_bias = gaussian(keys[9], (EXPERTS, D), 0.3, 2.0, (), jnp.float32)
    return dict(frames=frames, norm_gain=norm_gain, norm_bias=norm_bias, routes=routes, gate_codes=gate_codes, limits=limits, up_weight=up_weight, up_bias=up_bias, down_weight=down_weight, down_bias=down_bias)


epsilon = 1e-05

def layer_norm(frames, norm_gain, norm_bias):
    values = frames.astype(jnp.float32)
    center = lax.optimization_barrier(jnp.mean(values, axis=-1, keepdims=True))
    shifted = values - center
    spread = lax.optimization_barrier(jnp.mean(shifted * shifted, axis=-1, keepdims=True))
    return (shifted * lax.rsqrt(spread + epsilon) * norm_gain + norm_bias).astype(jnp.bfloat16)

def place_slots(routes_block, limits, expert_total, capacity):
    flat_routes = routes_block.reshape(-1)
    expert_ids = jnp.arange(expert_total, dtype=jnp.int32)
    expert_hits = (flat_routes[:, None] == expert_ids[None, :]).astype(jnp.int32)
    earlier = jnp.cumsum(expert_hits, axis=0).astype(jnp.int32) - expert_hits
    slot_rank = lax.optimization_barrier(jnp.sum(earlier * expert_hits, axis=1)).astype(jnp.int32)
    slot_bound = lax.optimization_barrier(jnp.sum(expert_hits * limits[None, :], axis=1)).astype(jnp.int32)
    kept_mask = (slot_rank < slot_bound).astype(jnp.int32)
    slot_index = jnp.minimum(flat_routes * capacity + slot_rank, expert_total * capacity - 1).astype(jnp.int32)
    slot_ids = jnp.arange(expert_total * capacity, dtype=jnp.int32)
    matches = (slot_index[None, :] == slot_ids[:, None]).astype(jnp.int32) * kept_mask[None, :]
    frame_ids = jnp.arange(flat_routes.shape[0], dtype=jnp.int32) // 2
    source_frame = lax.optimization_barrier(jnp.sum(matches * frame_ids[None, :], axis=1)).astype(jnp.int32)
    filled = lax.optimization_barrier(jnp.sum(matches, axis=1)).astype(jnp.int32)
    expert_loads = lax.optimization_barrier(jnp.sum(expert_hits * kept_mask[:, None], axis=0)).astype(jnp.int32)
    return (slot_index, kept_mask, source_frame, filled, expert_loads)

def fill_slots(normed_block, source_frame, filled):
    slot_rows = jnp.take(normed_block, source_frame, axis=0)
    return slot_rows * filled[:, None].astype(jnp.bfloat16)

def combine(frames_block, returned, slot_index, kept_mask, gate_block):
    code_values = gate_block.astype(jnp.float32)
    shares = code_values / lax.optimization_barrier(jnp.sum(code_values, axis=1, keepdims=True))
    weights = shares.reshape(-1) * kept_mask.astype(jnp.float32)
    picked = jnp.take(returned, slot_index, axis=0).astype(jnp.float32)
    weighted = (picked * weights[:, None]).reshape(frames_block.shape[0], 2, frames_block.shape[1])
    return (frames_block.astype(jnp.float32) + lax.optimization_barrier(jnp.sum(weighted, axis=1))).astype(jnp.bfloat16)

def expert_rows(slot_rows, w_up, b_up, w_down, b_down):
    preact = jnp.einsum('rd,sdf->srf', slot_rows.astype(jnp.float32), w_up.astype(jnp.float32)) + b_up[:, None, :]
    hidden = jax.nn.gelu(preact, approximate=False).astype(jnp.bfloat16)
    partial_out = jnp.einsum('srf,sfd->srd', hidden.astype(jnp.float32), w_down.astype(jnp.float32))
    rounded = lax.optimization_barrier(partial_out.astype(jnp.bfloat16)).astype(jnp.float32)
    return (lax.optimization_barrier(jnp.sum(rounded, axis=0)) + b_down).astype(jnp.bfloat16)

def reference(frames, norm_gain, norm_bias, routes, gate_codes, limits, up_weight, up_bias, down_weight, down_bias):
    blocks = N_DP * N_EXPERT
    normed = layer_norm(frames, norm_gain, norm_bias).reshape(blocks, TOK_DEV, D)

    def placer(routes_block):
        return place_slots(routes_block, limits, EXPERTS, CAP)
    slot_index, kept_mask, source_frame, filled, expert_loads = jax.vmap(placer)(routes.reshape(blocks, TOK_DEV, 2))
    sent_rows = jax.vmap(fill_slots)(normed, source_frame, filled)
    by_expert = sent_rows.reshape(blocks, EXPERTS, CAP, D).transpose(1, 0, 2, 3).reshape(EXPERTS, blocks * CAP, D)
    up_grouped = up_weight.reshape(EXPERTS, SHARDS, D, FF_DEV)
    upb_grouped = up_bias.reshape(EXPERTS, SHARDS, FF_DEV)
    down_grouped = down_weight.reshape(EXPERTS, SHARDS, FF_DEV, D)

    def one_expert(operands):
        return expert_rows(operands[0], operands[1], operands[2], operands[3], operands[4])
    outputs = lax.map(one_expert, (by_expert, up_grouped, upb_grouped, down_grouped, down_bias))
    returned = outputs.reshape(EXPERTS, blocks, CAP, D).transpose(1, 0, 2, 3).reshape(blocks, EXPERTS * CAP, D)
    mixed = jax.vmap(combine)(frames.reshape(blocks, TOK_DEV, D), returned, slot_index, kept_mask, gate_codes.reshape(blocks, TOK_DEV, 2))
    return (mixed.reshape(TOKENS, D), lax.optimization_barrier(jnp.sum(expert_loads, axis=0)).astype(jnp.int32))
```

```python
import random

import jax
import jax.numpy as jnp
from jax import lax
from jax.experimental import pallas as pl
from jax.experimental.pallas import tpu as pltpu
from jax.sharding import PartitionSpec as P

MESH = pl.DeviceIdType.MESH
EPS = 1e-05
D = 1024
FRAMES = 128
CAP = 16
PEERS = 32
CB = 256
CA = D - CB
CHUNKS = 4
PER = PEERS // CHUNKS
HALF = PER // 2
ROWS = 4 * PER * CAP
TILE = 256


def plane_order():
    rest = list(range(1, PEERS))
    random.Random(2).shuffle(rest)
    return [0] + rest


ORDER = plane_order()
OFFSETS = [((n // 2) % 4, n // 8, n % 2) for n in range(PEERS)]


def kernel(
    frames,
    gain,
    nbias,
    routes,
    codes,
    limits,
    up_hbm,
    up_b,
    down_hbm,
    down_b,
    mixed,
    load,
    up,
    down,
    slots_a,
    norm_b,
    slots_b,
    x_in,
    hid,
    part,
    t_r,
    t_l,
    g_l,
    g_r,
    e_out,
    ret_a,
    ret_b,
    y_out,
    y_in,
    info,
    cnt_out,
    cnt_in,
    brow,
    w_sem,
    send,
    r_a,
    r_b,
    r_info,
    r_nb,
    f_l,
    f_r,
    h_l,
    h_r,
    rt_r,
    rt_l,
    rg_l,
    rg_r,
    r_ra,
    r_rb,
    r_y,
    r_cnt,
):
    dp = lax.axis_index("dp")
    ex = lax.axis_index("expert")
    x, y = lax.rem(ex, 4), lax.div(ex, 4)
    z, c = lax.div(dp, 2), lax.rem(dp, 2)
    mine = dp * 4 + y

    def plane(n):
        dy, dz, dc = OFFSETS[n]
        return (
            lax.rem(z + dz, 4) * 2 + lax.rem(c + dc, 2),
            lax.rem(y + dy, 4) * 4 + x,
        )

    def source(n):
        dy, dz, dc = OFFSETS[n]
        return (
            lax.rem(z + 4 - dz, 4) * 2 + lax.rem(c + 2 - dc, 2),
            lax.rem(y + 4 - dy, 4) * 4 + x,
        )

    def along(k):
        return (dp, y * 4 + lax.rem(x + k, 4))

    def put(src, dst, s, r, where):
        pltpu.make_async_remote_copy(
            src, dst, s, r, device_id=where, device_id_type=MESH
        ).start()

    def arrived(ref, sem):
        pltpu.make_async_copy(ref, ref, sem).wait()

    barrier = pltpu.get_barrier_semaphore()
    for n in range(1, PEERS):
        pl.semaphore_signal(barrier, inc=1, device_id=plane(n), device_id_type=MESH)
    for k in range(1, 4):
        pl.semaphore_signal(barrier, inc=1, device_id=along(k), device_id_type=MESH)
    up_copy = pltpu.make_async_copy(up_hbm.at[0], up, w_sem.at[0])
    down_copy = pltpu.make_async_copy(down_hbm.at[0], down, w_sem.at[1])
    up_copy.start()
    down_copy.start()

    values = frames[...].astype(jnp.float32)
    center = jnp.mean(values, axis=-1, keepdims=True)
    shifted = values - center
    spread = jnp.mean(shifted * shifted, axis=-1, keepdims=True)
    normed = (shifted * lax.rsqrt(spread + EPS) * gain[...] + nbias[...]).astype(jnp.bfloat16)
    norm_b[0] = normed[:, CA:]

    chosen = routes[...]
    ids = lax.broadcasted_iota(jnp.int32, (FRAMES, FRAMES), 0)
    cols = lax.broadcasted_iota(jnp.int32, (FRAMES, FRAMES), 1)
    hit0 = (ids == chosen[0:1, :]).astype(jnp.float32)
    hit1 = (ids == chosen[1:2, :]).astype(jnp.float32)
    before = (ids < cols).astype(jnp.bfloat16)
    earlier = jnp.dot(
        (hit0 + hit1).astype(jnp.bfloat16), before, preferred_element_type=jnp.float32
    )
    rank = jnp.concatenate(
        [
            jnp.sum(earlier * hit0, axis=0, keepdims=True),
            jnp.sum(earlier * hit1, axis=0, keepdims=True),
        ],
        axis=0,
    ).astype(jnp.int32)
    bound = jnp.zeros((2, FRAMES), jnp.int32)
    for e in range(32):
        bound = jnp.where(chosen == e, limits[e], bound)
    kept = rank < bound
    dz = (lax.shift_right_logical(chosen, 3) - z + 4) & 3
    dc = ((lax.shift_right_logical(chosen, 2) & 1) - c + 2) & 1
    dy = ((chosen & 3) - y + 4) & 3
    spot = jnp.where(kept, ((dz * 4 + dy) * 2 + dc) * CAP + rank, -1)
    keptf = kept.astype(jnp.float32)
    taken = (hit0 * keptf[0:1, :] + hit1 * keptf[1:2, :]).astype(jnp.bfloat16)
    counts = lax.dot_general(
        jnp.ones((8, FRAMES), jnp.bfloat16),
        taken,
        (((1,), (1,)), ((), ())),
        preferred_element_type=jnp.float32,
    ).astype(jnp.int32)
    info[0, 0:2, :] = spot
    info[0, 2:4, :] = codes[...]
    info[0, 4:8, :] = counts[0:4, :]

    slot_ids = lax.broadcasted_iota(jnp.int32, (PEERS * CAP, FRAMES), 0)

    def gathered(k, rows):
        spots = info[k]
        pick = (slot_ids == spots[0:1, :]) | (slot_ids == spots[1:2, :])
        return (
            jnp.dot(
                pick.astype(jnp.float32).astype(jnp.bfloat16),
                rows,
                preferred_element_type=jnp.float32,
            )
            .astype(jnp.bfloat16)
            .reshape(PEERS, CAP, rows.shape[1])
        )

    slots_a[...] = gathered(0, normed[:, :CA])
    row = down_b[pl.ds(mine, 1), :]
    lane = lax.broadcasted_iota(jnp.int32, (1, D), 1)
    brow[...] = jnp.where(lane >= CA, row * 0.25, 0.0)

    pl.semaphore_wait(barrier, PEERS - 1 + 3)
    for k in range(1, 4):
        put(info.at[0], info.at[k], send.at[0], r_info.at[k - 1], along(k))
        put(norm_b.at[0], norm_b.at[k], send.at[1], r_nb.at[k - 1], along(k))
    for p in range(1, PEERS):
        n = ORDER[p]
        put(
            slots_a.at[n],
            x_in.at[0, p, :, pl.ds(0, CA)],
            send.at[2],
            r_a.at[p // PER],
            plane(n),
        )
    x_in[0, 0, :, :CA] = slots_a[0]

    slots_b[0] = gathered(0, normed[:, CA:])
    total = info[0, 4:5, :]
    for k in range(1, 4):
        arrived(info.at[k], r_info.at[k - 1])
        arrived(norm_b.at[k], r_nb.at[k - 1])
        slots_b[k] = gathered(k, norm_b[k])
        total = total + info[k, 4:5, :]
    cnt_out[...] = total
    for p in range(1, PEERS):
        n = ORDER[p]
        put(
            slots_b.at[:, n],
            x_in.at[:, p, :, pl.ds(CA, CB)],
            send.at[3],
            r_b.at[p // PER],
            plane(n),
        )
        put(cnt_out, cnt_in.at[n], send.at[4], r_cnt, plane(n))
    x_in[:, 0, :, CA:] = slots_b[:, 0]

    def chunk(j):
        return pl.ds(j * PER, PER)

    def first(j):
        return pl.ds(j * PER, HALF)

    def second(j):
        return pl.ds(j * PER + HALF, HALF)

    wide = pl.ds(0, CA)
    narrow = pl.ds(CA, CB)

    def own(j):
        begin = max(j * PER, 1)
        spots = pl.ds(begin, (j + 1) * PER - begin)
        arrived(x_in.at[0, spots, :, wide], r_a.at[j])
        put(
            x_in.at[0, chunk(j), :, wide],
            x_in.at[1, chunk(j), :, wide],
            send.at[5],
            f_l.at[j],
            along(1),
        )
        put(
            x_in.at[0, chunk(j), :, wide],
            x_in.at[3, chunk(j), :, wide],
            send.at[6],
            f_r.at[j],
            along(3),
        )

    def forward(j):
        arrived(x_in.at[1, chunk(j), :, wide], f_l.at[j])
        put(
            x_in.at[1, first(j), :, wide],
            x_in.at[2, first(j), :, wide],
            send.at[7],
            h_l.at[j],
            along(1),
        )
        arrived(x_in.at[3, chunk(j), :, wide], f_r.at[j])
        put(
            x_in.at[3, second(j), :, wide],
            x_in.at[2, second(j), :, wide],
            send.at[8],
            h_r.at[j],
            along(3),
        )

    def ready(j):
        begin = max(j * PER, 1)
        spots = pl.ds(begin, (j + 1) * PER - begin)
        arrived(x_in.at[:, spots, :, narrow], r_b.at[j])
        arrived(x_in.at[2, first(j), :, wide], h_l.at[j])
        arrived(x_in.at[2, second(j), :, wide], h_r.at[j])

    def project_up(j):
        def step(t, carry):
            lanes = pl.ds(pl.multiple_of(t * TILE, TILE), TILE)
            rows = x_in[:, j * PER : (j + 1) * PER].reshape(ROWS, D)
            pre = jnp.dot(rows, up[:, lanes], preferred_element_type=jnp.float32)
            pre = pre + up_b[:, lanes]
            act = 0.5 * pre * (1.0 + lax.erf(pre * 0.7071067811865476))
            hid[:, lanes] = act.astype(jnp.bfloat16)
            return carry

        lax.fori_loop(0, D // TILE, step, 0)

    def project_down(j):
        def step(t, carry):
            lanes = pl.ds(pl.multiple_of(t * TILE, TILE), TILE)
            out = jnp.dot(hid[...], down[:, lanes], preferred_element_type=jnp.float32)
            out = out + brow[:, lanes]
            part[:, j * PER : (j + 1) * PER, :, lanes] = out.astype(jnp.bfloat16).reshape(
                4, PER, CAP, TILE
            )
            return carry

        lax.fori_loop(0, D // TILE, step, 0)

    def give_back(j):
        put(part.at[2, first(j), :, wide], t_r.at[j], send.at[9], rt_r.at[j], along(1))
        put(part.at[2, second(j), :, wide], t_l.at[j], send.at[10], rt_l.at[j], along(3))
        put(part.at[3, second(j), :, wide], g_l.at[second(j)], send.at[11], rg_l.at[j], along(1))
        put(part.at[1, first(j), :, wide], g_r.at[first(j)], send.at[12], rg_r.at[j], along(3))
        for p in range(j * PER, (j + 1) * PER):
            if p:
                put(
                    part.at[:, p, :, narrow],
                    ret_b.at[:, ORDER[p]],
                    send.at[13],
                    r_rb,
                    source(ORDER[p]),
                )
            else:
                ret_b[:, 0] = part[:, 0, :, CA:]

    def add_on(j):
        arrived(t_r.at[j], rt_r.at[j])
        spots = slice(j * PER, j * PER + HALF)
        part[3, spots, :, :CA] = (
            part[3, spots, :, :CA].astype(jnp.float32) + t_r[j].astype(jnp.float32)
        ).astype(jnp.bfloat16)
        put(part.at[3, first(j), :, wide], g_l.at[first(j)], send.at[11], rg_l.at[j], along(1))
        arrived(t_l.at[j], rt_l.at[j])
        spots = slice(j * PER + HALF, (j + 1) * PER)
        part[1, spots, :, :CA] = (
            part[1, spots, :, :CA].astype(jnp.float32) + t_l[j].astype(jnp.float32)
        ).astype(jnp.bfloat16)
        put(part.at[1, second(j), :, wide], g_r.at[second(j)], send.at[12], rg_r.at[j], along(3))

    def finish(j):
        arrived(g_l.at[chunk(j)], rg_l.at[j])
        arrived(g_r.at[chunk(j)], rg_r.at[j])
        spots = slice(j * PER, (j + 1) * PER)
        bias = row[:, :CA].reshape(1, 1, CA)
        e_out[spots] = (
            part[0, spots, :, :CA].astype(jnp.float32)
            + g_l[spots].astype(jnp.float32)
            + g_r[spots].astype(jnp.float32)
            + bias
        ).astype(jnp.bfloat16)
        for p in range(j * PER, (j + 1) * PER):
            if p:
                put(e_out.at[p], ret_a.at[ORDER[p]], send.at[14], r_ra, source(ORDER[p]))
            else:
                ret_a[0] = e_out[0]

    own(0)
    own(1)
    forward(0)
    own(2)
    forward(1)
    own(3)
    up_copy.wait()
    down_copy.wait()
    ready(0)
    project_up(0)
    forward(2)
    project_down(0)
    give_back(0)
    forward(3)
    ready(1)
    project_up(1)
    add_on(0)
    project_down(1)
    give_back(1)
    finish(0)
    ready(2)
    project_up(2)
    add_on(1)
    project_down(2)
    give_back(2)
    finish(1)
    ready(3)
    project_up(3)
    add_on(2)
    project_down(3)
    give_back(3)
    finish(2)
    add_on(3)
    finish(3)

    arrived(cnt_in.at[pl.ds(1, PEERS - 1)], r_cnt)
    cnt_in[0] = cnt_out[...]
    load[...] = jnp.sum(cnt_in[...], axis=0)[:, :32]

    slot_cols = lax.broadcasted_iota(jnp.int32, (FRAMES, PEERS * CAP), 1)

    def combined(k, rows):
        table = jnp.concatenate([info[k], jnp.zeros((FRAMES - 8, FRAMES), jnp.int32)], axis=0)
        turned = jnp.transpose(table.astype(jnp.float32))
        code0, code1 = turned[:, 2:3], turned[:, 3:4]
        weight0 = code0 / (code0 + code1)
        weight1 = code1 / (code0 + code1)
        spots = turned.astype(jnp.int32)
        pick0 = (slot_cols == spots[:, 0:1]).astype(jnp.float32).astype(jnp.bfloat16)
        pick1 = (slot_cols == spots[:, 1:2]).astype(jnp.float32).astype(jnp.bfloat16)
        out0 = jnp.dot(pick0, rows, preferred_element_type=jnp.float32)
        out1 = jnp.dot(pick1, rows, preferred_element_type=jnp.float32)
        return out0 * weight0 + out1 * weight1

    arrived(ret_b.at[:, pl.ds(1, PEERS - 1)], r_rb)
    for k in range(1, 4):
        y_out[k - 1] = combined(k, ret_b[k].reshape(PEERS * CAP, CB)).astype(jnp.bfloat16)
        put(y_out.at[k - 1], y_in.at[k - 1], send.at[15], r_y.at[k - 1], along(4 - k))
    own_b = combined(0, ret_b[0].reshape(PEERS * CAP, CB))
    arrived(ret_a.at[pl.ds(1, PEERS - 1)], r_ra)
    own_a = combined(0, ret_a[...].reshape(PEERS * CAP, CA))
    mixed[:, :CA] = (frames[:, :CA].astype(jnp.float32) + own_a).astype(jnp.bfloat16)
    for k in range(1, 4):
        arrived(y_in.at[k - 1], r_y.at[k - 1])
        own_b = own_b + y_in[k - 1].astype(jnp.float32)
    mixed[:, CA:] = (frames[:, CA:].astype(jnp.float32) + own_b).astype(jnp.bfloat16)

    rest = pl.ds(1, PEERS - 1)
    some = pl.ds(1, 3)
    halves = pl.ds(0, PEERS // 2)
    arrived(info.at[some], send.at[0])
    arrived(norm_b.at[some], send.at[1])
    arrived(slots_a.at[rest], send.at[2])
    arrived(slots_b.at[:, rest], send.at[3])
    arrived(cnt_in.at[rest], send.at[4])
    arrived(e_out, send.at[5])
    arrived(e_out, send.at[6])
    arrived(e_out.at[halves], send.at[7])
    arrived(e_out.at[halves], send.at[8])
    arrived(e_out.at[halves], send.at[9])
    arrived(e_out.at[halves], send.at[10])
    arrived(e_out, send.at[11])
    arrived(e_out, send.at[12])
    arrived(slots_b.at[:, rest], send.at[13])
    arrived(slots_a.at[rest], send.at[14])
    arrived(y_out, send.at[15])


def per_device(frames, gain, nbias, routes, codes, limits, up_w, up_b, down_w, down_b):
    vmem = pl.BlockSpec(memory_space=pltpu.VMEM)
    hbm = pl.BlockSpec(memory_space=pl.ANY)
    smem = pl.BlockSpec(memory_space=pltpu.SMEM)
    bf16, f32, i32 = jnp.bfloat16, jnp.float32, jnp.int32
    dma = pltpu.SemaphoreType.DMA
    mixed, load = pl.pallas_call(
        kernel,
        out_shape=(
            jax.ShapeDtypeStruct((FRAMES, D), bf16),
            jax.ShapeDtypeStruct((1, 32), i32),
        ),
        in_specs=[vmem, vmem, vmem, vmem, vmem, smem, hbm, vmem, hbm, vmem],
        out_specs=(vmem, vmem),
        scratch_shapes=[
            pltpu.VMEM((D, D), bf16),
            pltpu.VMEM((D, D), bf16),
            pltpu.VMEM((PEERS, CAP, CA), bf16),
            pltpu.VMEM((4, FRAMES, CB), bf16),
            pltpu.VMEM((4, PEERS, CAP, CB), bf16),
            pltpu.VMEM((4, PEERS, CAP, D), bf16),
            pltpu.VMEM((ROWS, D), bf16),
            pltpu.VMEM((4, PEERS, CAP, D), bf16),
            pltpu.VMEM((CHUNKS, HALF, CAP, CA), bf16),
            pltpu.VMEM((CHUNKS, HALF, CAP, CA), bf16),
            pltpu.VMEM((PEERS, CAP, CA), bf16),
            pltpu.VMEM((PEERS, CAP, CA), bf16),
            pltpu.VMEM((PEERS, CAP, CA), bf16),
            pltpu.VMEM((PEERS, CAP, CA), bf16),
            pltpu.VMEM((4, PEERS, CAP, CB), bf16),
            pltpu.VMEM((3, FRAMES, CB), bf16),
            pltpu.VMEM((3, FRAMES, CB), bf16),
            pltpu.VMEM((4, 8, FRAMES), i32),
            pltpu.VMEM((1, FRAMES), i32),
            pltpu.VMEM((PEERS, 1, FRAMES), i32),
            pltpu.VMEM((1, D), f32),
            dma((2,)),
            dma((16,)),
            dma((CHUNKS,)),
            dma((CHUNKS,)),
            dma((3,)),
            dma((3,)),
            dma((CHUNKS,)),
            dma((CHUNKS,)),
            dma((CHUNKS,)),
            dma((CHUNKS,)),
            dma((CHUNKS,)),
            dma((CHUNKS,)),
            dma((CHUNKS,)),
            dma((CHUNKS,)),
            dma,
            dma,
            dma((3,)),
            dma,
        ],
        compiler_params=pltpu.CompilerParams(
            collective_id=0, has_side_effects=True, vmem_limit_bytes=56 << 20
        ),
        name="moe",
    )(
        frames,
        gain.reshape(1, D),
        nbias.reshape(1, D),
        routes.T,
        codes.T,
        limits,
        up_w,
        up_b,
        down_w,
        down_b,
    )
    return mixed, load.reshape(32)


def solution(mesh):
    both = ("dp", "expert")
    in_specs = (
        P(both, None),
        P(),
        P(),
        P(both, None),
        P(both, None),
        P(),
        P(both, None, None),
        P(both, None),
        P(both, None, None),
        P(),
    )
    out_specs = (P(both, None), P())
    return jax.shard_map(
        per_device, mesh=mesh, in_specs=in_specs, out_specs=out_specs, check_vma=False
    )
```

```python
import random

import jax
import jax.numpy as jnp
from jax import lax
from jax.experimental import pallas as pl
from jax.experimental.pallas import tpu as pltpu
from jax.sharding import PartitionSpec as P

MESH = pl.DeviceIdType.MESH
EPS = 1e-05
D = 1024
FRAMES = 128
CAP = 16
PEERS = 32
CB = 384
CA = D - CB
SIZES = [8, 8, 8, 8]
CHUNKS = len(SIZES)
STARTS = [sum(SIZES[:j]) for j in range(CHUNKS + 1)]
CHUNK_OF = [j for j in range(CHUNKS) for _ in range(SIZES[j])]
TILE = 256


def plane_order():
    rest = list(range(1, PEERS))
    random.Random(5).shuffle(rest)
    return [0] + rest


ORDER = plane_order()
SCHEDULE = (
    "own0 gath0 send0 own1 fwd0 own2 fwd1 own3 wts0 "
    "ready0 up0 fwd2 down0 give0 ready1 up1 fwd3 down1 give1 add0 "
    "ready2 up2 down2 give2 add1 ready3 up3 down3 give3 fin0 add2 fin1 add3 fin2 fin3"
)
OFFSETS = [((n // 2) % 4, n // 8, n % 2) for n in range(PEERS)]


def kernel(
    frames_hbm,
    gain_hbm,
    nbias_hbm,
    routes_hbm,
    codes_hbm,
    limits_hbm,
    up_hbm,
    up_b_hbm,
    down_hbm,
    down_b_hbm,
    mixed,
    load,
    frames,
    gain,
    nbias,
    routes,
    codes,
    limits,
    up_b,
    down_b,
    up,
    down,
    slots_a,
    norm_b,
    slots_b,
    x_in,
    hid,
    part,
    t_r,
    t_l,
    g_l,
    g_r,
    e_out,
    ret_a,
    ret_b,
    y_out,
    y_in,
    info,
    cnt_out,
    cnt_in,
    brow,
    w_sem,
    send,
    r_a,
    r_b,
    r_info,
    r_nb,
    f_l,
    f_r,
    h_l,
    h_r,
    rt_r,
    rt_l,
    rg_l,
    rg_r,
    r_ra,
    r_rb,
    r_y,
    r_cnt,
):
    dp = lax.axis_index("dp")
    ex = lax.axis_index("expert")
    x, y = lax.rem(ex, 4), lax.div(ex, 4)
    z, c = lax.div(dp, 2), lax.rem(dp, 2)
    mine = dp * 4 + y

    def plane(n):
        dy, dz, dc = OFFSETS[n]
        return (
            lax.rem(z + dz, 4) * 2 + lax.rem(c + dc, 2),
            lax.rem(y + dy, 4) * 4 + x,
        )

    def source(n):
        dy, dz, dc = OFFSETS[n]
        return (
            lax.rem(z + 4 - dz, 4) * 2 + lax.rem(c + 2 - dc, 2),
            lax.rem(y + 4 - dy, 4) * 4 + x,
        )

    def along(k):
        return (dp, y * 4 + lax.rem(x + k, 4))

    def put(src, dst, s, r, where):
        pltpu.make_async_remote_copy(
            src, dst, s, r, device_id=where, device_id_type=MESH
        ).start()

    def arrived(ref, sem):
        pltpu.make_async_copy(ref, ref, sem).wait()

    with jax.named_scope("greet"):
        barrier = pltpu.get_barrier_semaphore()
        for n in range(1, PEERS):
            pl.semaphore_signal(barrier, inc=1, device_id=plane(n), device_id_type=MESH)
        for k in range(1, 4):
            pl.semaphore_signal(barrier, inc=1, device_id=along(k), device_id_type=MESH)
        loads = [
            pltpu.make_async_copy(src, dst, w_sem.at[i])
            for i, (src, dst) in enumerate(
                [
                    (frames_hbm, frames),
                    (gain_hbm, gain),
                    (nbias_hbm, nbias),
                    (routes_hbm, routes),
                    (codes_hbm, codes),
                    (limits_hbm, limits),
                    (down_b_hbm.at[pl.ds(pl.multiple_of(lax.div(mine, 8) * 8, 8), 8)], down_b),
                    (up_b_hbm, up_b),
                    (up_hbm.at[0], up),
                    (down_hbm.at[0], down),
                ]
            )
        ]
        for copy in loads:
            copy.start()
        for copy in loads[:6]:
            copy.wait()

    with jax.named_scope("norm"):
        values = frames[...].astype(jnp.float32)
        center = jnp.mean(values, axis=-1, keepdims=True)
        shifted = values - center
        spread = jnp.mean(shifted * shifted, axis=-1, keepdims=True)
        normed = (shifted * lax.rsqrt(spread + EPS) * gain[...] + nbias[...]).astype(jnp.bfloat16)
        norm_b[0] = normed[:, CA:]

    with jax.named_scope("route"):
        chosen = routes[...]
        ids = lax.broadcasted_iota(jnp.int32, (FRAMES, FRAMES), 0)
        cols = lax.broadcasted_iota(jnp.int32, (FRAMES, FRAMES), 1)
        hit0 = (ids == chosen[0:1, :]).astype(jnp.float32)
        hit1 = (ids == chosen[1:2, :]).astype(jnp.float32)
        before = (ids < cols).astype(jnp.bfloat16)
        earlier = jnp.dot(
            (hit0 + hit1).astype(jnp.bfloat16), before, preferred_element_type=jnp.float32
        )
        rank = jnp.concatenate(
            [
                jnp.sum(earlier * hit0, axis=0, keepdims=True),
                jnp.sum(earlier * hit1, axis=0, keepdims=True),
            ],
            axis=0,
        ).astype(jnp.int32)
        bound = jnp.zeros((2, FRAMES), jnp.int32)
        for e in range(32):
            bound = jnp.where(chosen == e, limits[e], bound)
        kept = rank < bound
        dz = (lax.shift_right_logical(chosen, 3) - z + 4) & 3
        dc = ((lax.shift_right_logical(chosen, 2) & 1) - c + 2) & 1
        dy = ((chosen & 3) - y + 4) & 3
        spot = jnp.where(kept, ((dz * 4 + dy) * 2 + dc) * CAP + rank, -1)
        keptf = kept.astype(jnp.float32)
        taken = (hit0 * keptf[0:1, :] + hit1 * keptf[1:2, :]).astype(jnp.bfloat16)
        counts = lax.dot_general(
            jnp.ones((8, FRAMES), jnp.bfloat16),
            taken,
            (((1,), (1,)), ((), ())),
            preferred_element_type=jnp.float32,
        ).astype(jnp.int32)
        info[0, 0:2, :] = spot
        info[0, 2:4, :] = codes[...]
        info[0, 4:8, :] = counts[0:4, :]

    slot_ids = lax.broadcasted_iota(jnp.int32, (PEERS * CAP, FRAMES), 0)

    def gathered(k, rows):
        spots = info[k]
        pick = (slot_ids == spots[0:1, :]) | (slot_ids == spots[1:2, :])
        return (
            jnp.dot(
                pick.astype(jnp.float32).astype(jnp.bfloat16),
                rows,
                preferred_element_type=jnp.float32,
            )
            .astype(jnp.bfloat16)
            .reshape(PEERS, CAP, rows.shape[1])
        )

    with jax.named_scope("gather"):
        slots_a[...] = gathered(0, normed[:, :CA])
        loads[6].wait()
        row = down_b[pl.ds(lax.rem(mine, 8), 1), :]
        lane = lax.broadcasted_iota(jnp.int32, (1, D), 1)
        brow[...] = jnp.where(lane >= CA, row * 0.25, 0.0)

    with jax.named_scope("met"):
        pl.semaphore_wait(barrier, PEERS - 1 + 3)
    with jax.named_scope("send_a"):
        for k in range(1, 4):
            put(info.at[0], info.at[k], send.at[0], r_info.at[k - 1], along(k))
            put(norm_b.at[0], norm_b.at[k], send.at[1], r_nb.at[k - 1], along(k))
        for p in range(1, PEERS):
            n = ORDER[p]
            put(
                slots_a.at[n],
                x_in.at[0, p, :, pl.ds(0, CA)],
                send.at[2],
                r_a.at[CHUNK_OF[p]],
                plane(n),
            )
        x_in[0, 0, :, :CA] = slots_a[0]

    def chunk(j):
        return pl.ds(STARTS[j], SIZES[j])

    def first(j):
        return pl.ds(STARTS[j], SIZES[j] // 2)

    def second(j):
        return pl.ds(STARTS[j] + SIZES[j] // 2, SIZES[j] // 2)

    def halves(j):
        return pl.ds(STARTS[j] // 2, SIZES[j] // 2)

    def remote(j):
        begin = max(STARTS[j], 1)
        return pl.ds(begin, STARTS[j + 1] - begin)

    wide = pl.ds(0, CA)
    narrow = pl.ds(CA, CB)

    def own(j):
        arrived(x_in.at[0, remote(j), :, wide], r_a.at[j])
        put(
            x_in.at[0, chunk(j), :, wide],
            x_in.at[1, chunk(j), :, wide],
            send.at[5],
            f_l.at[j],
            along(1),
        )
        put(
            x_in.at[0, chunk(j), :, wide],
            x_in.at[3, chunk(j), :, wide],
            send.at[6],
            f_r.at[j],
            along(3),
        )

    def forward(j):
        arrived(x_in.at[1, chunk(j), :, wide], f_l.at[j])
        put(
            x_in.at[1, first(j), :, wide],
            x_in.at[2, first(j), :, wide],
            send.at[7],
            h_l.at[j],
            along(1),
        )
        arrived(x_in.at[3, chunk(j), :, wide], f_r.at[j])
        put(
            x_in.at[3, second(j), :, wide],
            x_in.at[2, second(j), :, wide],
            send.at[8],
            h_r.at[j],
            along(3),
        )

    def ready(j):
        arrived(x_in.at[:, remote(j), :, narrow], r_b.at[j])
        arrived(x_in.at[2, first(j), :, wide], h_l.at[j])
        arrived(x_in.at[2, second(j), :, wide], h_r.at[j])

    def project_up(j):
        def step(t, carry):
            lanes = pl.ds(pl.multiple_of(t * TILE, TILE), TILE)
            rows = x_in[:, STARTS[j] : STARTS[j + 1]].reshape(4 * SIZES[j] * CAP, D)
            pre = jnp.dot(rows, up[:, lanes], preferred_element_type=jnp.float32)
            pre = pre + up_b[:, lanes]
            act = 0.5 * pre * (1.0 + lax.erf(pre * 0.7071067811865476))
            hid[: 4 * SIZES[j] * CAP, lanes] = act.astype(jnp.bfloat16)
            return carry

        lax.fori_loop(0, D // TILE, step, 0)

    def project_down(j):
        def step(t, carry):
            lanes = pl.ds(pl.multiple_of(t * TILE, TILE), TILE)
            out = jnp.dot(hid[: 4 * SIZES[j] * CAP], down[:, lanes], preferred_element_type=jnp.float32)
            out = out + brow[:, lanes]
            part[:, STARTS[j] : STARTS[j + 1], :, lanes] = out.astype(jnp.bfloat16).reshape(
                4, SIZES[j], CAP, TILE
            )
            return carry

        lax.fori_loop(0, D // TILE, step, 0)

    def give_back(j):
        put(part.at[2, first(j), :, wide], t_r.at[halves(j)], send.at[9], rt_r.at[j], along(1))
        put(part.at[2, second(j), :, wide], t_l.at[halves(j)], send.at[10], rt_l.at[j], along(3))
        put(part.at[3, second(j), :, wide], g_l.at[second(j)], send.at[11], rg_l.at[j], along(1))
        put(part.at[1, first(j), :, wide], g_r.at[first(j)], send.at[12], rg_r.at[j], along(3))
        for p in range(STARTS[j], STARTS[j + 1]):
            if p:
                put(
                    part.at[:, p, :, narrow],
                    ret_b.at[:, ORDER[p]],
                    send.at[13],
                    r_rb,
                    source(ORDER[p]),
                )
            else:
                ret_b[:, 0] = part[:, 0, :, CA:]

    def add_on(j):
        arrived(t_r.at[halves(j)], rt_r.at[j])
        spots = slice(STARTS[j], STARTS[j] + SIZES[j] // 2)
        part[3, spots, :, :CA] = (
            part[3, spots, :, :CA].astype(jnp.float32) + t_r[STARTS[j] // 2 : STARTS[j + 1] // 2].astype(jnp.float32)
        ).astype(jnp.bfloat16)
        put(part.at[3, first(j), :, wide], g_l.at[first(j)], send.at[11], rg_l.at[j], along(1))
        arrived(t_l.at[halves(j)], rt_l.at[j])
        spots = slice(STARTS[j] + SIZES[j] // 2, STARTS[j + 1])
        part[1, spots, :, :CA] = (
            part[1, spots, :, :CA].astype(jnp.float32) + t_l[STARTS[j] // 2 : STARTS[j + 1] // 2].astype(jnp.float32)
        ).astype(jnp.bfloat16)
        put(part.at[1, second(j), :, wide], g_r.at[second(j)], send.at[12], rg_r.at[j], along(3))

    def finish(j):
        arrived(g_l.at[chunk(j)], rg_l.at[j])
        arrived(g_r.at[chunk(j)], rg_r.at[j])
        spots = slice(STARTS[j], STARTS[j + 1])
        bias = row[:, :CA].reshape(1, 1, CA)
        e_out[spots] = (
            part[0, spots, :, :CA].astype(jnp.float32)
            + g_l[spots].astype(jnp.float32)
            + g_r[spots].astype(jnp.float32)
            + bias
        ).astype(jnp.bfloat16)
        for p in range(STARTS[j], STARTS[j + 1]):
            if p:
                put(e_out.at[p], ret_a.at[ORDER[p]], send.at[14], r_ra, source(ORDER[p]))
            else:
                ret_a[0] = e_out[0]

    def blocks_b(j):
        slots_b[0] = gathered(0, normed[:, CA:])
        total = info[0, 4:5, :]
        for k in range(1, 4):
            arrived(info.at[k], r_info.at[k - 1])
            arrived(norm_b.at[k], r_nb.at[k - 1])
            slots_b[k] = gathered(k, norm_b[k])
            total = total + info[k, 4:5, :]
        cnt_out[...] = total

    def send_b(j):
        for p in range(1, PEERS):
            n = ORDER[p]
            put(
                slots_b.at[:, n],
                x_in.at[:, p, :, pl.ds(CA, CB)],
                send.at[3],
                r_b.at[CHUNK_OF[p]],
                plane(n),
            )
            put(cnt_out, cnt_in.at[n], send.at[4], r_cnt, plane(n))
        x_in[:, 0, :, CA:] = slots_b[:, 0]

    def weights(j):
        for copy in loads[7:]:
            copy.wait()

    steps = {
        "gath": blocks_b,
        "send": send_b,
        "wts": weights,
        "own": own,
        "fwd": forward,
        "ready": ready,
        "up": project_up,
        "down": project_down,
        "give": give_back,
        "add": add_on,
        "fin": finish,
    }
    for entry in SCHEDULE.split():
        with jax.named_scope(entry):
            steps[entry[:-1]](int(entry[-1]))

    with jax.named_scope("load"):
        arrived(cnt_in.at[pl.ds(1, PEERS - 1)], r_cnt)
        cnt_in[0] = cnt_out[...]
        load[...] = jnp.sum(cnt_in[...], axis=0)[:, :32]

    slot_cols = lax.broadcasted_iota(jnp.int32, (FRAMES, PEERS * CAP), 1)

    def combined(k, rows):
        table = jnp.concatenate([info[k], jnp.zeros((FRAMES - 8, FRAMES), jnp.int32)], axis=0)
        turned = jnp.transpose(table.astype(jnp.float32))
        code0, code1 = turned[:, 2:3], turned[:, 3:4]
        weight0 = code0 / (code0 + code1)
        weight1 = code1 / (code0 + code1)
        spots = turned.astype(jnp.int32)
        pick0 = (slot_cols == spots[:, 0:1]).astype(jnp.float32).astype(jnp.bfloat16)
        pick1 = (slot_cols == spots[:, 1:2]).astype(jnp.float32).astype(jnp.bfloat16)
        out0 = jnp.dot(pick0, rows, preferred_element_type=jnp.float32)
        out1 = jnp.dot(pick1, rows, preferred_element_type=jnp.float32)
        return out0 * weight0 + out1 * weight1

    with jax.named_scope("blocks"):
        with jax.named_scope("wait_rb"):
            arrived(ret_b.at[:, pl.ds(1, PEERS - 1)], r_rb)
        for k in range(1, 4):
            y_out[k - 1] = combined(k, ret_b[k].reshape(PEERS * CAP, CB)).astype(jnp.bfloat16)
            put(y_out.at[k - 1], y_in.at[k - 1], send.at[15], r_y.at[k - 1], along(4 - k))
    with jax.named_scope("own_rows"):
        own_b = combined(0, ret_b[0].reshape(PEERS * CAP, CB))
        with jax.named_scope("wait_ra"):
            arrived(ret_a.at[pl.ds(1, PEERS - 1)], r_ra)
        own_a = combined(0, ret_a[...].reshape(PEERS * CAP, CA))
    with jax.named_scope("mix"):
        mixed[:, :CA] = (frames[:, :CA].astype(jnp.float32) + own_a).astype(jnp.bfloat16)
        for k in range(1, 4):
            arrived(y_in.at[k - 1], r_y.at[k - 1])
            own_b = own_b + y_in[k - 1].astype(jnp.float32)
        mixed[:, CA:] = (frames[:, CA:].astype(jnp.float32) + own_b).astype(jnp.bfloat16)

    with jax.named_scope("sent"):
        rest = pl.ds(1, PEERS - 1)
        some = pl.ds(1, 3)
        half = pl.ds(0, PEERS // 2)
        arrived(info.at[some], send.at[0])
        arrived(norm_b.at[some], send.at[1])
        arrived(slots_a.at[rest], send.at[2])
        arrived(slots_b.at[:, rest], send.at[3])
        arrived(cnt_in.at[rest], send.at[4])
        arrived(e_out, send.at[5])
        arrived(e_out, send.at[6])
        arrived(e_out.at[half], send.at[7])
        arrived(e_out.at[half], send.at[8])
        arrived(e_out.at[half], send.at[9])
        arrived(e_out.at[half], send.at[10])
        arrived(e_out, send.at[11])
        arrived(e_out, send.at[12])
        arrived(slots_b.at[:, rest], send.at[13])
        arrived(slots_a.at[rest], send.at[14])
        arrived(y_out, send.at[15])


def per_device(frames, gain, nbias, routes, codes, limits, up_w, up_b, down_w, down_b):
    vmem = pl.BlockSpec(memory_space=pltpu.VMEM)
    hbm = pl.BlockSpec(memory_space=pltpu.HBM)
    bf16, f32, i32 = jnp.bfloat16, jnp.float32, jnp.int32
    dma = pltpu.SemaphoreType.DMA
    mixed, load = pl.pallas_call(
        kernel,
        out_shape=(
            jax.ShapeDtypeStruct((FRAMES, D), bf16),
            jax.ShapeDtypeStruct((1, 32), i32),
        ),
        in_specs=[hbm] * 10,
        out_specs=(vmem, vmem),
        scratch_shapes=[
            pltpu.VMEM((FRAMES, D), bf16),
            pltpu.VMEM((1, D), f32),
            pltpu.VMEM((1, D), f32),
            pltpu.VMEM((2, FRAMES), i32),
            pltpu.VMEM((2, FRAMES), i32),
            pltpu.SMEM((32,), i32),
            pltpu.VMEM((1, D), f32),
            pltpu.VMEM((8, D), f32),
            pltpu.VMEM((D, D), bf16),
            pltpu.VMEM((D, D), bf16),
            pltpu.VMEM((PEERS, CAP, CA), bf16),
            pltpu.VMEM((4, FRAMES, CB), bf16),
            pltpu.VMEM((4, PEERS, CAP, CB), bf16),
            pltpu.VMEM((4, PEERS, CAP, D), bf16),
            pltpu.VMEM((4 * max(SIZES) * CAP, D), bf16),
            pltpu.VMEM((4, PEERS, CAP, D), bf16),
            pltpu.VMEM((PEERS // 2, CAP, CA), bf16),
            pltpu.VMEM((PEERS // 2, CAP, CA), bf16),
            pltpu.VMEM((PEERS, CAP, CA), bf16),
            pltpu.VMEM((PEERS, CAP, CA), bf16),
            pltpu.VMEM((PEERS, CAP, CA), bf16),
            pltpu.VMEM((PEERS, CAP, CA), bf16),
            pltpu.VMEM((4, PEERS, CAP, CB), bf16),
            pltpu.VMEM((3, FRAMES, CB), bf16),
            pltpu.VMEM((3, FRAMES, CB), bf16),
            pltpu.VMEM((4, 8, FRAMES), i32),
            pltpu.VMEM((1, FRAMES), i32),
            pltpu.VMEM((PEERS, 1, FRAMES), i32),
            pltpu.VMEM((1, D), f32),
            dma((10,)),
            dma((16,)),
            dma((CHUNKS,)),
            dma((CHUNKS,)),
            dma((3,)),
            dma((3,)),
            dma((CHUNKS,)),
            dma((CHUNKS,)),
            dma((CHUNKS,)),
            dma((CHUNKS,)),
            dma((CHUNKS,)),
            dma((CHUNKS,)),
            dma((CHUNKS,)),
            dma((CHUNKS,)),
            dma,
            dma,
            dma((3,)),
            dma,
        ],
        compiler_params=pltpu.CompilerParams(
            collective_id=0, has_side_effects=True, vmem_limit_bytes=30 << 20
        ),
        name="moe",
    )(
        *[
            pltpu.with_memory_space_constraint(value, pltpu.HBM)
            for value in (
                frames,
                gain.reshape(1, D),
                nbias.reshape(1, D),
                routes.T,
                codes.T,
                limits,
                up_w,
                up_b,
                down_w,
                down_b,
            )
        ],
    )
    return mixed, load.reshape(32)


def solution(mesh):
    both = ("dp", "expert")
    in_specs = (
        P(both, None),
        P(),
        P(),
        P(both, None),
        P(both, None),
        P(),
        P(both, None, None),
        P(both, None),
        P(both, None, None),
        P(),
    )
    out_specs = (P(both, None), P())
    return jax.shard_map(
        per_device, mesh=mesh, in_specs=in_specs, out_specs=out_specs, check_vma=False
    )
```

```python
import jax
import jax.numpy as jnp
from jax import lax
from jax.experimental import pallas as pl
from jax.experimental.pallas import tpu as pltpu
from jax.sharding import PartitionSpec as P

MESH = pl.DeviceIdType.MESH
EPS = 1e-05
D = 1024
FRAMES = 128
CAP = 16
PEERS = 32
CB = 384
CA = D - CB
RB = 384
RA = D - RB
SIZES = [8, 8, 8, 8]
CHUNKS = len(SIZES)
STARTS = [sum(SIZES[:j]) for j in range(CHUNKS + 1)]
CHUNK_OF = [j for j in range(CHUNKS) for _ in range(SIZES[j])]
TILE = 256


OFFSETS = [((n // 2) % 4, n // 8, n % 2) for n in range(PEERS)]


ORDER = [
    0, 6, 8, 30, 14, 26, 2, 18, 15, 13, 1, 27, 17, 31, 28, 10,
    21, 25, 4, 19, 23, 16, 12, 5, 7, 9, 3, 29, 11, 22, 20, 24,
]
SCHEDULE = [
    "sa0", "sa1", "sa2", "sa3", "own0", "gath0", "sb0", "sb1",
    "sb2", "sb3", "cnt0", "own1", "fwd0", "own2", "fwd1", "own3",
    "wts0", "ready0", "up0", "fwd2", "down0", "give0", "ready1", "up1",
    "fwd3", "down1", "give1", "ready2", "up2", "add0", "down2", "give2",
    "ready3", "up3", "add1", "down3", "give3", "add2", "fin0", "fin1",
    "add3", "fin2", "fin3",
]


def kernel(
    frames_hbm,
    gain_hbm,
    nbias_hbm,
    routes_hbm,
    codes_hbm,
    limits_hbm,
    up_hbm,
    up_b_hbm,
    down_hbm,
    down_b_hbm,
    mixed,
    load,
    frames,
    gain,
    nbias,
    routes,
    codes,
    limits,
    up_b,
    down_b,
    up,
    down,
    slots_a,
    norm_b,
    slots_b,
    x_in,
    hid,
    part,
    t_r,
    t_l,
    g_l,
    g_r,
    e_out,
    ret_a,
    ret_b,
    y_out,
    y_in,
    info,
    cnt_out,
    cnt_in,
    brow,
    w_sem,
    send,
    r_a,
    r_b,
    r_info,
    r_nb,
    f_l,
    f_r,
    h_l,
    h_r,
    rt_r,
    rt_l,
    rg_l,
    rg_r,
    r_ra,
    r_rb,
    r_y,
    r_cnt,
):
    dp = lax.axis_index("dp")
    ex = lax.axis_index("expert")
    x, y = lax.rem(ex, 4), lax.div(ex, 4)
    z, c = lax.div(dp, 2), lax.rem(dp, 2)
    mine = dp * 4 + y

    def plane(n):
        dy, dz, dc = OFFSETS[n]
        return (
            lax.rem(z + dz, 4) * 2 + lax.rem(c + dc, 2),
            lax.rem(y + dy, 4) * 4 + x,
        )

    def source(n):
        dy, dz, dc = OFFSETS[n]
        return (
            lax.rem(z + 4 - dz, 4) * 2 + lax.rem(c + 2 - dc, 2),
            lax.rem(y + 4 - dy, 4) * 4 + x,
        )

    def along(k):
        return (dp, y * 4 + lax.rem(x + k, 4))

    def put(src, dst, s, r, where):
        pltpu.make_async_remote_copy(
            src, dst, s, r, device_id=where, device_id_type=MESH
        ).start()

    def arrived(ref, sem):
        pltpu.make_async_copy(ref, ref, sem).wait()

    with jax.named_scope("greet"):
        loads = [
            pltpu.make_async_copy(src, dst, w_sem.at[i])
            for i, (src, dst) in enumerate(
                [
                    (frames_hbm, frames),
                    (gain_hbm, gain),
                    (nbias_hbm, nbias),
                    (routes_hbm, routes),
                    (codes_hbm, codes),
                    (limits_hbm, limits),
                    (down_b_hbm.at[pl.ds(pl.multiple_of(lax.div(mine, 8) * 8, 8), 8)], down_b),
                    (up_b_hbm, up_b),
                    (up_hbm.at[0], up),
                    (down_hbm.at[0], down),
                ]
            )
        ]
        for copy in loads:
            copy.start()
        barrier = pltpu.get_barrier_semaphore()
        for n in range(1, PEERS):
            pl.semaphore_signal(barrier, inc=1, device_id=plane(n), device_id_type=MESH)
        for k in range(1, 4):
            pl.semaphore_signal(barrier, inc=1, device_id=along(k), device_id_type=MESH)
        for copy in loads[3:6]:
            copy.wait()

    with jax.named_scope("route"):
        chosen = routes[...]
        ids = lax.broadcasted_iota(jnp.int32, (FRAMES, FRAMES), 0)
        cols = lax.broadcasted_iota(jnp.int32, (FRAMES, FRAMES), 1)
        hit0 = (ids == chosen[0:1, :]).astype(jnp.float32)
        hit1 = (ids == chosen[1:2, :]).astype(jnp.float32)
        before = (ids < cols).astype(jnp.bfloat16)
        earlier = jnp.dot(
            (hit0 + hit1).astype(jnp.bfloat16), before, preferred_element_type=jnp.float32
        )
        rank = jnp.concatenate(
            [
                jnp.sum(earlier * hit0, axis=0, keepdims=True),
                jnp.sum(earlier * hit1, axis=0, keepdims=True),
            ],
            axis=0,
        ).astype(jnp.int32)
        bound = jnp.zeros((2, FRAMES), jnp.int32)
        for e in range(32):
            bound = jnp.where(chosen == e, limits[e], bound)
        kept = rank < bound
        dz = (lax.shift_right_logical(chosen, 3) - z + 4) & 3
        dc = ((lax.shift_right_logical(chosen, 2) & 1) - c + 2) & 1
        dy = ((chosen & 3) - y + 4) & 3
        spot = jnp.where(kept, ((dz * 4 + dy) * 2 + dc) * CAP + rank, -1)
        keptf = kept.astype(jnp.float32)
        taken = (hit0 * keptf[0:1, :] + hit1 * keptf[1:2, :]).astype(jnp.bfloat16)
        counts = lax.dot_general(
            jnp.ones((8, FRAMES), jnp.bfloat16),
            taken,
            (((1,), (1,)), ((), ())),
            preferred_element_type=jnp.float32,
        ).astype(jnp.int32)
        info[0, 0:2, :] = spot
        info[0, 2:4, :] = codes[...]
        info[0, 4:8, :] = counts[0:4, :]

    with jax.named_scope("norm"):
        for copy in loads[:3]:
            copy.wait()
        values = frames[...].astype(jnp.float32)
        center = jnp.mean(values, axis=-1, keepdims=True)
        shifted = values - center
        spread = jnp.mean(shifted * shifted, axis=-1, keepdims=True)
        normed = (shifted * lax.rsqrt(spread + EPS) * gain[...] + nbias[...]).astype(jnp.bfloat16)
        norm_b[0] = normed[:, CA:]

    slot_ids = lax.broadcasted_iota(jnp.int32, (PEERS * CAP, FRAMES), 0)

    def gathered(k, rows):
        spots = info[k]
        pick = (slot_ids == spots[0:1, :]) | (slot_ids == spots[1:2, :])
        return (
            jnp.dot(
                pick.astype(jnp.float32).astype(jnp.bfloat16),
                rows,
                preferred_element_type=jnp.float32,
            )
            .astype(jnp.bfloat16)
            .reshape(PEERS, CAP, rows.shape[1])
        )

    with jax.named_scope("gather"):
        slots_a[...] = gathered(0, normed[:, :CA])
        loads[6].wait()
        row = down_b[pl.ds(lax.rem(mine, 8), 1), :]
        lane = lax.broadcasted_iota(jnp.int32, (1, D), 1)
        brow[...] = jnp.where(lane >= RA, row * 0.25, 0.0)

    with jax.named_scope("met"):
        pl.semaphore_wait(barrier, PEERS - 1 + 3)
    with jax.named_scope("send_a"):
        for k in range(1, 4):
            put(info.at[0], info.at[k], send.at[0], r_info.at[k - 1], along(k))
            put(norm_b.at[0], norm_b.at[k], send.at[1], r_nb.at[k - 1], along(k))
        x_in[0, 0, :, :CA] = slots_a[0]

    def chunk(j):
        return pl.ds(STARTS[j], SIZES[j])

    def first(j):
        return pl.ds(STARTS[j], SIZES[j] // 2)

    def second(j):
        return pl.ds(STARTS[j] + SIZES[j] // 2, SIZES[j] // 2)

    def halves(j):
        return pl.ds(STARTS[j] // 2, SIZES[j] // 2)

    def remote(j):
        begin = max(STARTS[j], 1)
        return pl.ds(begin, STARTS[j + 1] - begin)

    wide = pl.ds(0, CA)
    narrow = pl.ds(CA, CB)
    wide_back = pl.ds(0, RA)
    narrow_back = pl.ds(RA, RB)

    def own(j):
        arrived(x_in.at[0, remote(j), :, wide], r_a.at[j])
        put(
            x_in.at[0, chunk(j), :, wide],
            x_in.at[1, chunk(j), :, wide],
            send.at[5],
            f_l.at[j],
            along(1),
        )
        put(
            x_in.at[0, chunk(j), :, wide],
            x_in.at[3, chunk(j), :, wide],
            send.at[6],
            f_r.at[j],
            along(3),
        )

    def forward(j):
        arrived(x_in.at[1, chunk(j), :, wide], f_l.at[j])
        put(
            x_in.at[1, first(j), :, wide],
            x_in.at[2, first(j), :, wide],
            send.at[7],
            h_l.at[j],
            along(1),
        )
        arrived(x_in.at[3, chunk(j), :, wide], f_r.at[j])
        put(
            x_in.at[3, second(j), :, wide],
            x_in.at[2, second(j), :, wide],
            send.at[8],
            h_r.at[j],
            along(3),
        )

    def ready(j):
        arrived(x_in.at[:, remote(j), :, narrow], r_b.at[j])
        arrived(x_in.at[2, first(j), :, wide], h_l.at[j])
        arrived(x_in.at[2, second(j), :, wide], h_r.at[j])

    def project_up(j):
        def step(t, carry):
            lanes = pl.ds(pl.multiple_of(t * TILE, TILE), TILE)
            rows = x_in[:, STARTS[j] : STARTS[j + 1]].reshape(4 * SIZES[j] * CAP, D)
            pre = jnp.dot(rows, up[:, lanes], preferred_element_type=jnp.float32)
            pre = pre + up_b[:, lanes]
            act = 0.5 * pre * (1.0 + lax.erf(pre * 0.7071067811865476))
            hid[: 4 * SIZES[j] * CAP, lanes] = act.astype(jnp.bfloat16)
            return carry

        lax.fori_loop(0, D // TILE, step, 0)

    def project_down(j):
        def step(t, carry):
            lanes = pl.ds(pl.multiple_of(t * TILE, TILE), TILE)
            out = jnp.dot(hid[: 4 * SIZES[j] * CAP], down[:, lanes], preferred_element_type=jnp.float32)
            out = out + brow[:, lanes]
            part[:, STARTS[j] : STARTS[j + 1], :, lanes] = out.astype(jnp.bfloat16).reshape(
                4, SIZES[j], CAP, TILE
            )
            return carry

        lax.fori_loop(0, D // TILE, step, 0)

    def give_back(j):
        put(part.at[2, first(j), :, wide_back], t_r.at[halves(j)], send.at[9], rt_r.at[j], along(1))
        put(part.at[2, second(j), :, wide_back], t_l.at[halves(j)], send.at[10], rt_l.at[j], along(3))
        put(part.at[3, second(j), :, wide_back], g_l.at[second(j)], send.at[11], rg_l.at[j], along(1))
        put(part.at[1, first(j), :, wide_back], g_r.at[first(j)], send.at[12], rg_r.at[j], along(3))
        for p in range(STARTS[j], STARTS[j + 1]):
            if p:
                put(
                    part.at[:, p, :, narrow_back],
                    ret_b.at[:, ORDER[p]],
                    send.at[13],
                    r_rb,
                    source(ORDER[p]),
                )
            else:
                ret_b[:, 0] = part[:, 0, :, RA:]

    def add_on(j):
        arrived(t_r.at[halves(j)], rt_r.at[j])
        spots = slice(STARTS[j], STARTS[j] + SIZES[j] // 2)
        part[3, spots, :, :RA] = (
            part[3, spots, :, :RA].astype(jnp.float32) + t_r[STARTS[j] // 2 : STARTS[j + 1] // 2].astype(jnp.float32)
        ).astype(jnp.bfloat16)
        put(part.at[3, first(j), :, wide_back], g_l.at[first(j)], send.at[11], rg_l.at[j], along(1))
        arrived(t_l.at[halves(j)], rt_l.at[j])
        spots = slice(STARTS[j] + SIZES[j] // 2, STARTS[j + 1])
        part[1, spots, :, :RA] = (
            part[1, spots, :, :RA].astype(jnp.float32) + t_l[STARTS[j] // 2 : STARTS[j + 1] // 2].astype(jnp.float32)
        ).astype(jnp.bfloat16)
        put(part.at[1, second(j), :, wide_back], g_r.at[second(j)], send.at[12], rg_r.at[j], along(3))

    def finish(j):
        arrived(g_l.at[chunk(j)], rg_l.at[j])
        arrived(g_r.at[chunk(j)], rg_r.at[j])
        spots = slice(STARTS[j], STARTS[j + 1])
        bias = row[:, :RA].reshape(1, 1, RA)
        e_out[spots] = (
            part[0, spots, :, :RA].astype(jnp.float32)
            + g_l[spots].astype(jnp.float32)
            + g_r[spots].astype(jnp.float32)
            + bias
        ).astype(jnp.bfloat16)
        for p in range(STARTS[j], STARTS[j + 1]):
            if p:
                put(e_out.at[p], ret_a.at[ORDER[p]], send.at[14], r_ra, source(ORDER[p]))
            else:
                ret_a[0] = e_out[0]

    def blocks_b(j):
        slots_b[0] = gathered(0, normed[:, CA:])
        total = info[0, 4:5, :]
        for k in range(1, 4):
            arrived(info.at[k], r_info.at[k - 1])
            arrived(norm_b.at[k], r_nb.at[k - 1])
            slots_b[k] = gathered(k, norm_b[k])
            total = total + info[k, 4:5, :]
        cnt_out[...] = total
        x_in[:, 0, :, CA:] = slots_b[:, 0]

    def send_a(j):
        for p in range(max(STARTS[j], 1), STARTS[j + 1]):
            n = ORDER[p]
            put(
                slots_a.at[n],
                x_in.at[0, p, :, pl.ds(0, CA)],
                send.at[2],
                r_a.at[j],
                plane(n),
            )

    def send_b(j):
        for p in range(max(STARTS[j], 1), STARTS[j + 1]):
            n = ORDER[p]
            put(
                slots_b.at[:, n],
                x_in.at[:, p, :, pl.ds(CA, CB)],
                send.at[3],
                r_b.at[j],
                plane(n),
            )

    def send_counts(j):
        for n in range(1, PEERS):
            put(cnt_out, cnt_in.at[n], send.at[4], r_cnt, plane(n))

    def weights(j):
        for copy in loads[7:]:
            copy.wait()

    steps = {
        "gath": blocks_b,
        "sa": send_a,
        "sb": send_b,
        "cnt": send_counts,
        "wts": weights,
        "own": own,
        "fwd": forward,
        "ready": ready,
        "up": project_up,
        "down": project_down,
        "give": give_back,
        "add": add_on,
        "fin": finish,
    }
    for entry in SCHEDULE:
        with jax.named_scope(entry):
            steps[entry[:-1]](int(entry[-1]))

    with jax.named_scope("load"):
        arrived(cnt_in.at[pl.ds(1, PEERS - 1)], r_cnt)
        cnt_in[0] = cnt_out[...]
        load[...] = jnp.sum(cnt_in[...], axis=0)[:, :32]

    slot_cols = lax.broadcasted_iota(jnp.int32, (FRAMES, PEERS * CAP), 1)

    def picks(k):
        table = jnp.concatenate([info[k], jnp.zeros((FRAMES - 8, FRAMES), jnp.int32)], axis=0)
        turned = jnp.transpose(table.astype(jnp.float32))
        code0, code1 = turned[:, 2:3], turned[:, 3:4]
        weight0 = code0 / (code0 + code1)
        weight1 = code1 / (code0 + code1)
        spots = turned.astype(jnp.int32)
        pick0 = (slot_cols == spots[:, 0:1]).astype(jnp.float32).astype(jnp.bfloat16)
        pick1 = (slot_cols == spots[:, 1:2]).astype(jnp.float32).astype(jnp.bfloat16)
        return pick0, pick1, weight0, weight1

    def weighted(found, rows):
        pick0, pick1, weight0, weight1 = found
        out0 = jnp.dot(pick0, rows, preferred_element_type=jnp.float32)
        out1 = jnp.dot(pick1, rows, preferred_element_type=jnp.float32)
        return out0 * weight0 + out1 * weight1

    with jax.named_scope("blocks"):
        with jax.named_scope("wait_rb"):
            arrived(ret_b.at[:, pl.ds(1, PEERS - 1)], r_rb)
        for k in range(1, 4):
            y_out[k - 1] = weighted(picks(k), ret_b[k].reshape(PEERS * CAP, RB)).astype(jnp.bfloat16)
            put(y_out.at[k - 1], y_in.at[k - 1], send.at[15], r_y.at[k - 1], along(4 - k))
    with jax.named_scope("own_rows"):
        mine_at = picks(0)
        own_b = weighted(mine_at, ret_b[0].reshape(PEERS * CAP, RB))
        with jax.named_scope("wait_ra"):
            arrived(ret_a.at[pl.ds(1, PEERS - 1)], r_ra)
        own_a = weighted(mine_at, ret_a[...].reshape(PEERS * CAP, RA))
    with jax.named_scope("mix"):
        mixed[:, :RA] = (frames[:, :RA].astype(jnp.float32) + own_a).astype(jnp.bfloat16)
        for k in range(1, 4):
            arrived(y_in.at[k - 1], r_y.at[k - 1])
            own_b = own_b + y_in[k - 1].astype(jnp.float32)
        mixed[:, RA:] = (frames[:, RA:].astype(jnp.float32) + own_b).astype(jnp.bfloat16)

    with jax.named_scope("sent"):
        rest = pl.ds(1, PEERS - 1)
        some = pl.ds(1, 3)
        half = pl.ds(0, PEERS // 2)
        arrived(info.at[some], send.at[0])
        arrived(norm_b.at[some], send.at[1])
        arrived(slots_a.at[rest], send.at[2])
        arrived(slots_b.at[:, rest], send.at[3])
        arrived(cnt_in.at[rest], send.at[4])
        arrived(x_in.at[0, :, :, wide], send.at[5])
        arrived(x_in.at[0, :, :, wide], send.at[6])
        arrived(x_in.at[0, half, :, wide], send.at[7])
        arrived(x_in.at[0, half, :, wide], send.at[8])
        arrived(e_out.at[half], send.at[9])
        arrived(e_out.at[half], send.at[10])
        arrived(e_out, send.at[11])
        arrived(e_out, send.at[12])
        arrived(ret_b.at[:, rest], send.at[13])
        arrived(e_out.at[rest], send.at[14])
        arrived(y_out, send.at[15])


def finish_kernel(mixed_in, load_in, mixed, load, sems):
    copies = [
        pltpu.make_async_copy(mixed_in, mixed, sems.at[0]),
        pltpu.make_async_copy(load_in, load, sems.at[1]),
    ]
    for copy in copies:
        copy.start()
    for copy in copies:
        copy.wait()


def per_device(frames, gain, nbias, routes, codes, limits, up_w, up_b, down_w, down_b):
    vmem = pl.BlockSpec(memory_space=pltpu.VMEM)
    hbm = pl.BlockSpec(memory_space=pltpu.HBM)
    bf16, f32, i32 = jnp.bfloat16, jnp.float32, jnp.int32
    dma = pltpu.SemaphoreType.DMA
    mixed, load = pl.pallas_call(
        kernel,
        out_shape=(
            jax.ShapeDtypeStruct((FRAMES, D), bf16),
            jax.ShapeDtypeStruct((1, 32), i32),
        ),
        in_specs=[hbm] * 10,
        out_specs=(vmem, vmem),
        scratch_shapes=[
            pltpu.VMEM((FRAMES, D), bf16),
            pltpu.VMEM((1, D), f32),
            pltpu.VMEM((1, D), f32),
            pltpu.VMEM((2, FRAMES), i32),
            pltpu.VMEM((2, FRAMES), i32),
            pltpu.SMEM((32,), i32),
            pltpu.VMEM((1, D), f32),
            pltpu.VMEM((8, D), f32),
            pltpu.VMEM((D, D), bf16),
            pltpu.VMEM((D, D), bf16),
            pltpu.VMEM((PEERS, CAP, CA), bf16),
            pltpu.VMEM((4, FRAMES, CB), bf16),
            pltpu.VMEM((4, PEERS, CAP, CB), bf16),
            pltpu.VMEM((4, PEERS, CAP, D), bf16),
            pltpu.VMEM((4 * max(SIZES) * CAP, D), bf16),
            pltpu.VMEM((4, PEERS, CAP, D), bf16),
            pltpu.VMEM((PEERS // 2, CAP, RA), bf16),
            pltpu.VMEM((PEERS // 2, CAP, RA), bf16),
            pltpu.VMEM((PEERS, CAP, RA), bf16),
            pltpu.VMEM((PEERS, CAP, RA), bf16),
            pltpu.VMEM((PEERS, CAP, RA), bf16),
            pltpu.VMEM((PEERS, CAP, RA), bf16),
            pltpu.VMEM((4, PEERS, CAP, RB), bf16),
            pltpu.VMEM((3, FRAMES, RB), bf16),
            pltpu.VMEM((3, FRAMES, RB), bf16),
            pltpu.VMEM((4, 8, FRAMES), i32),
            pltpu.VMEM((1, FRAMES), i32),
            pltpu.VMEM((PEERS, 1, FRAMES), i32),
            pltpu.VMEM((1, D), f32),
            dma((10,)),
            dma((16,)),
            dma((CHUNKS,)),
            dma((CHUNKS,)),
            dma((3,)),
            dma((3,)),
            dma((CHUNKS,)),
            dma((CHUNKS,)),
            dma((CHUNKS,)),
            dma((CHUNKS,)),
            dma((CHUNKS,)),
            dma((CHUNKS,)),
            dma((CHUNKS,)),
            dma((CHUNKS,)),
            dma,
            dma,
            dma((3,)),
            dma,
        ],
        compiler_params=pltpu.CompilerParams(
            collective_id=0, has_side_effects=True, vmem_limit_bytes=30 << 20
        ),
        name="moe",
    )(
        *[
            pltpu.with_memory_space_constraint(value, pltpu.HBM)
            for value in (
                frames,
                gain.reshape(1, D),
                nbias.reshape(1, D),
                routes.T,
                codes.T,
                limits,
                up_w,
                up_b,
                down_w,
                down_b,
            )
        ],
    )
    mixed, load = pl.pallas_call(
        finish_kernel,
        out_shape=(
            jax.ShapeDtypeStruct((FRAMES, D), bf16),
            jax.ShapeDtypeStruct((1, 32), i32),
        ),
        in_specs=[vmem, vmem],
        out_specs=(hbm, hbm),
        scratch_shapes=[dma((2,))],
        compiler_params=pltpu.CompilerParams(vmem_limit_bytes=1 << 20),
        name="store",
    )(mixed, load)
    return mixed, load.reshape(32)


def solution(mesh):
    both = ("dp", "expert")
    in_specs = (
        P(both, None),
        P(),
        P(),
        P(both, None),
        P(both, None),
        P(),
        P(both, None, None),
        P(both, None),
        P(both, None, None),
        P(),
    )
    out_specs = (P(both, None), P())
    return jax.shard_map(
        per_device, mesh=mesh, in_specs=in_specs, out_specs=out_specs, check_vma=False
    )
```

```python
import jax
import jax.numpy as jnp
from jax import lax
from jax.experimental import pallas as pl
from jax.experimental.pallas import tpu as pltpu
from jax.sharding import PartitionSpec as P

MESH = pl.DeviceIdType.MESH
EPS = 1e-05
D = 1024
FRAMES = 128
CAP = 16
PEERS = 32
CB = 384
CA = D - CB
RB = 384
RA = D - RB
SIZES = [8, 8, 8, 8]
CHUNKS = len(SIZES)
LOAD_SEM = [0, 0, 1, 2, 3, 3, 3, 4, 5, 5]
STARTS = [sum(SIZES[:j]) for j in range(CHUNKS + 1)]
CHUNK_OF = [j for j in range(CHUNKS) for _ in range(SIZES[j])]
TILE = 256


OFFSETS = [((n // 2) % 4, n // 8, n % 2) for n in range(PEERS)]


ORDER = [
    0, 18, 30, 14, 26, 6, 8, 2, 15, 13, 1, 27, 17, 31, 28, 10,
    21, 25, 4, 19, 23, 16, 12, 5, 20, 29, 22, 11, 7, 9, 3, 24,
]
SCHEDULE = [
    "sa0", "sa1", "sa2", "sa3", "own0", "gath0", "sb0", "sb1",
    "sb2", "sb3", "cnt0", "own1", "fwd0", "own2", "fwd1", "own3",
    "wts0", "ready0", "up0", "fwd2", "down0", "give0", "ready1", "up1",
    "fwd3", "down1", "give1", "ready2", "up2", "add0", "down2", "give2",
    "ready3", "up3", "add1", "down3", "give3", "fin0", "add2", "fin1",
    "add3", "fin2", "blk0", "fin3",
]


def kernel(
    frames_hbm,
    gain_hbm,
    nbias_hbm,
    routes_hbm,
    codes_hbm,
    limits_hbm,
    up_hbm,
    up_b_hbm,
    down_hbm,
    down_b_hbm,
    mixed,
    load,
    frames,
    vectors,
    pairs,
    limits,
    down_b,
    weights,
    slots_a,
    norm_b,
    slots_b,
    x_in,
    hid,
    part,
    t,
    g,
    e_out,
    ret_a,
    ret_b,
    y_out,
    y_in,
    info,
    cnt_out,
    cnt_in,
    brow,
    w_sem,
    send,
    r_a,
    r_b,
    r_info,
    r_nb,
    f_l,
    f_r,
    r_h,
    r_t,
    r_g,
    r_ra,
    r_rb,
    r_y,
    r_cnt,
):
    dp = lax.axis_index("dp")
    ex = lax.axis_index("expert")
    x, y = lax.rem(ex, 4), lax.div(ex, 4)
    z, c = lax.div(dp, 2), lax.rem(dp, 2)
    mine = dp * 4 + y

    zs = [lax.rem(z + k, 4) * 2 for k in range(4)]
    ys = [lax.rem(y + k, 4) * 4 + x for k in range(4)]
    cs = [c, 1 - c]

    def plane(n):
        dy, dz, dc = OFFSETS[n]
        return (zs[dz] + cs[dc], ys[dy])

    def source(n):
        dy, dz, dc = OFFSETS[n]
        return (zs[-dz] + cs[dc], ys[-dy])

    def along(k):
        return (dp, y * 4 + lax.rem(x + k, 4))

    def put(src, dst, s, r, where):
        pltpu.make_async_remote_copy(
            src, dst, s, r, device_id=where, device_id_type=MESH
        ).start()

    def arrived(ref, sem):
        pltpu.make_async_copy(ref, ref, sem).wait()

    with jax.named_scope("greet"):
        loads = [
            pltpu.make_async_copy(src, dst, w_sem.at[LOAD_SEM[i]])
            for i, (src, dst) in enumerate(
                [
                    (routes_hbm, pairs.at[0]),
                    (codes_hbm, pairs.at[1]),
                    (limits_hbm, limits),
                    (frames_hbm, frames),
                    (gain_hbm, vectors.at[0]),
                    (nbias_hbm, vectors.at[1]),
                    (up_b_hbm, vectors.at[2]),
                    (down_b_hbm.at[pl.ds(pl.multiple_of(lax.div(mine, 8) * 8, 8), 8)], down_b),
                    (up_hbm.at[0], weights.at[0]),
                    (down_hbm.at[0], weights.at[1]),
                ]
            )
        ]
        for copy in loads:
            copy.start()
        barrier = pltpu.get_barrier_semaphore()
        for n in range(1, PEERS):
            pl.semaphore_signal(barrier, inc=1, device_id=plane(n), device_id_type=MESH)
        for k in range(1, 4):
            pl.semaphore_signal(barrier, inc=1, device_id=along(k), device_id_type=MESH)
        arrived(pairs, w_sem.at[0])
        loads[2].wait()

    with jax.named_scope("route"):
        chosen = pairs[0]
        ids = lax.broadcasted_iota(jnp.int32, (FRAMES, FRAMES), 0)
        cols = lax.broadcasted_iota(jnp.int32, (FRAMES, FRAMES), 1)
        hit0 = (ids == chosen[0:1, :]).astype(jnp.float32)
        hit1 = (ids == chosen[1:2, :]).astype(jnp.float32)
        before = (ids < cols).astype(jnp.bfloat16)
        earlier = jnp.dot(
            (hit0 + hit1).astype(jnp.bfloat16), before, preferred_element_type=jnp.float32
        )
        rank = jnp.concatenate(
            [
                jnp.sum(earlier * hit0, axis=0, keepdims=True),
                jnp.sum(earlier * hit1, axis=0, keepdims=True),
            ],
            axis=0,
        ).astype(jnp.int32)
        bound = jnp.zeros((2, FRAMES), jnp.int32)
        for e in range(32):
            bound = jnp.where(chosen == e, limits[e], bound)
        kept = rank < bound
        dz = (lax.shift_right_logical(chosen, 3) - z + 4) & 3
        dc = ((lax.shift_right_logical(chosen, 2) & 1) - c + 2) & 1
        dy = ((chosen & 3) - y + 4) & 3
        spot = jnp.where(kept, ((dz * 4 + dy) * 2 + dc) * CAP + rank, -1)
        keptf = kept.astype(jnp.float32)
        taken = (hit0 * keptf[0:1, :] + hit1 * keptf[1:2, :]).astype(jnp.bfloat16)
        counts = lax.dot_general(
            jnp.ones((8, FRAMES), jnp.bfloat16),
            taken,
            (((1,), (1,)), ((), ())),
            preferred_element_type=jnp.float32,
        ).astype(jnp.int32)
        info[0, 0:2, :] = spot
        info[0, 2:4, :] = pairs[1]
        info[0, 4:8, :] = counts[0:4, :]

    with jax.named_scope("norm"):
        loads[3].wait()
        arrived(vectors, w_sem.at[3])
        values = frames[...].astype(jnp.float32)
        center = jnp.mean(values, axis=-1, keepdims=True)
        shifted = values - center
        spread = jnp.mean(shifted * shifted, axis=-1, keepdims=True)
        normed = (shifted * lax.rsqrt(spread + EPS) * vectors[0] + vectors[1]).astype(jnp.bfloat16)
        norm_b[0] = normed[:, CA:]

    slot_ids = lax.broadcasted_iota(jnp.int32, (PEERS * CAP, FRAMES), 0)

    def gathered(k, rows):
        spots = info[k]
        pick = (slot_ids == spots[0:1, :]) | (slot_ids == spots[1:2, :])
        return (
            jnp.dot(
                pick.astype(jnp.float32).astype(jnp.bfloat16),
                rows,
                preferred_element_type=jnp.float32,
            )
            .astype(jnp.bfloat16)
            .reshape(PEERS, CAP, rows.shape[1])
        )

    with jax.named_scope("gather"):
        slots_a[...] = gathered(0, normed[:, :CA])
        loads[7].wait()
        row = down_b[pl.ds(lax.rem(mine, 8), 1), :]
        lane = lax.broadcasted_iota(jnp.int32, (1, D), 1)
        brow[...] = jnp.where(lane >= RA, row * 0.25, 0.0)
        x_in[0, 0, :, :CA] = slots_a[0]

    with jax.named_scope("met"):
        pl.semaphore_wait(barrier, PEERS - 1 + 3)
    with jax.named_scope("send_a"):
        for k in range(1, 4):
            put(info.at[0], info.at[k], send.at[0], r_info, along(k))
            put(norm_b.at[0], norm_b.at[k], send.at[1], r_nb.at[k - 1], along(k))

    def chunk(j):
        return pl.ds(STARTS[j], SIZES[j])

    def first(j):
        return pl.ds(STARTS[j], SIZES[j] // 2)

    def second(j):
        return pl.ds(STARTS[j] + SIZES[j] // 2, SIZES[j] // 2)

    def halves(j):
        return pl.ds(STARTS[j] // 2, SIZES[j] // 2)

    def remote(j):
        begin = max(STARTS[j], 1)
        return pl.ds(begin, STARTS[j + 1] - begin)

    wide = pl.ds(0, CA)
    narrow = pl.ds(CA, CB)
    wide_back = pl.ds(0, RA)
    narrow_back = pl.ds(RA, RB)

    def own(j):
        arrived(x_in.at[0, remote(j), :, wide], r_a.at[j])
        put(
            x_in.at[0, chunk(j), :, wide],
            x_in.at[1, chunk(j), :, wide],
            send.at[5],
            f_l.at[j],
            along(1),
        )
        put(
            x_in.at[0, chunk(j), :, wide],
            x_in.at[3, chunk(j), :, wide],
            send.at[5],
            f_r.at[j],
            along(3),
        )

    def forward(j):
        arrived(x_in.at[1, chunk(j), :, wide], f_l.at[j])
        put(
            x_in.at[1, first(j), :, wide],
            x_in.at[2, first(j), :, wide],
            send.at[5],
            r_h.at[j],
            along(1),
        )
        arrived(x_in.at[3, chunk(j), :, wide], f_r.at[j])
        put(
            x_in.at[3, second(j), :, wide],
            x_in.at[2, second(j), :, wide],
            send.at[5],
            r_h.at[j],
            along(3),
        )

    def ready(j):
        arrived(x_in.at[:, remote(j), :, narrow], r_b.at[j])
        arrived(x_in.at[2, chunk(j), :, wide], r_h.at[j])

    def project_up(j):
        def step(t, carry):
            lanes = pl.ds(pl.multiple_of(t * TILE, TILE), TILE)
            rows = x_in[:, STARTS[j] : STARTS[j + 1]].reshape(4 * SIZES[j] * CAP, D)
            pre = jnp.dot(rows, weights[0, :, lanes], preferred_element_type=jnp.float32)
            pre = pre + vectors[2, :, lanes]
            act = 0.5 * pre * (1.0 + lax.erf(pre * 0.7071067811865476))
            hid[: 4 * SIZES[j] * CAP, lanes] = act.astype(jnp.bfloat16)
            return carry

        lax.fori_loop(0, D // TILE, step, 0)

    def project_down(j):
        def step(t, carry):
            lanes = pl.ds(pl.multiple_of(t * TILE, TILE), TILE)
            out = jnp.dot(hid[: 4 * SIZES[j] * CAP], weights[1, :, lanes], preferred_element_type=jnp.float32)
            out = out + brow[:, lanes]
            part[:, STARTS[j] : STARTS[j + 1], :, lanes] = out.astype(jnp.bfloat16).reshape(
                4, SIZES[j], CAP, TILE
            )
            return carry

        lax.fori_loop(0, D // TILE, step, 0)

    def give_back(j):
        put(part.at[2, first(j), :, wide_back], t.at[0, halves(j)], send.at[6], r_t.at[j], along(1))
        put(part.at[2, second(j), :, wide_back], t.at[1, halves(j)], send.at[6], r_t.at[j], along(3))
        put(part.at[3, second(j), :, wide_back], g.at[0, second(j)], send.at[6], r_g.at[j], along(1))
        put(part.at[1, first(j), :, wide_back], g.at[1, first(j)], send.at[6], r_g.at[j], along(3))
        for p in range(STARTS[j], STARTS[j + 1]):
            if p:
                put(
                    part.at[:, p, :, narrow_back],
                    ret_b.at[:, ORDER[p]],
                    send.at[7],
                    r_rb,
                    source(ORDER[p]),
                )
            else:
                ret_b[:, 0] = part[:, 0, :, RA:]

    def add_on(j):
        arrived(t.at[:, halves(j)], r_t.at[j])
        spots = slice(STARTS[j], STARTS[j] + SIZES[j] // 2)
        part[3, spots, :, :RA] = (
            part[3, spots, :, :RA].astype(jnp.float32) + t[0, STARTS[j] // 2 : STARTS[j + 1] // 2].astype(jnp.float32)
        ).astype(jnp.bfloat16)
        put(part.at[3, first(j), :, wide_back], g.at[0, first(j)], send.at[6], r_g.at[j], along(1))
        spots = slice(STARTS[j] + SIZES[j] // 2, STARTS[j + 1])
        part[1, spots, :, :RA] = (
            part[1, spots, :, :RA].astype(jnp.float32) + t[1, STARTS[j] // 2 : STARTS[j + 1] // 2].astype(jnp.float32)
        ).astype(jnp.bfloat16)
        put(part.at[1, second(j), :, wide_back], g.at[1, second(j)], send.at[6], r_g.at[j], along(3))

    def finish(j):
        arrived(g.at[:, chunk(j)], r_g.at[j])
        spots = slice(STARTS[j], STARTS[j + 1])
        bias = row[:, :RA].reshape(1, 1, RA)
        e_out[spots] = (
            part[0, spots, :, :RA].astype(jnp.float32)
            + g[0, spots].astype(jnp.float32)
            + g[1, spots].astype(jnp.float32)
            + bias
        ).astype(jnp.bfloat16)
        for p in range(STARTS[j], STARTS[j + 1]):
            if p:
                put(e_out.at[p], ret_a.at[ORDER[p]], send.at[8], r_ra, source(ORDER[p]))
            else:
                ret_a[0] = e_out[0]

    def blocks_b(j):
        slots_b[0] = gathered(0, normed[:, CA:])
        total = info[0, 4:5, :]
        arrived(info.at[pl.ds(1, 3)], r_info)
        for k in range(1, 4):
            arrived(norm_b.at[k], r_nb.at[k - 1])
            slots_b[k] = gathered(k, norm_b[k])
            total = total + info[k, 4:5, :]
        cnt_out[...] = total
        x_in[:, 0, :, CA:] = slots_b[:, 0]

    def send_a(j):
        for p in range(max(STARTS[j], 1), STARTS[j + 1]):
            n = ORDER[p]
            put(
                slots_a.at[n],
                x_in.at[0, p, :, pl.ds(0, CA)],
                send.at[2],
                r_a.at[j],
                plane(n),
            )

    def send_b(j):
        for p in range(max(STARTS[j], 1), STARTS[j + 1]):
            n = ORDER[p]
            put(
                slots_b.at[:, n],
                x_in.at[:, p, :, pl.ds(CA, CB)],
                send.at[3],
                r_b.at[j],
                plane(n),
            )

    def send_counts(j):
        for n in range(1, PEERS):
            put(cnt_out, cnt_in.at[n], send.at[4], r_cnt, plane(n))

    def weights_in(j):
        arrived(weights, w_sem.at[5])

    slot_cols = lax.broadcasted_iota(jnp.int32, (FRAMES, PEERS * CAP), 1)

    def picks(k):
        table = jnp.concatenate([info[k], jnp.zeros((FRAMES - 8, FRAMES), jnp.int32)], axis=0)
        turned = jnp.transpose(table.astype(jnp.float32))
        code0, code1 = turned[:, 2:3], turned[:, 3:4]
        weight0 = code0 / (code0 + code1)
        weight1 = code1 / (code0 + code1)
        spots = turned.astype(jnp.int32)
        pick0 = (slot_cols == spots[:, 0:1]).astype(jnp.float32).astype(jnp.bfloat16)
        pick1 = (slot_cols == spots[:, 1:2]).astype(jnp.float32).astype(jnp.bfloat16)
        return pick0, pick1, weight0, weight1

    def weighted(found, rows):
        pick0, pick1, weight0, weight1 = found
        out0 = jnp.dot(pick0, rows, preferred_element_type=jnp.float32)
        out1 = jnp.dot(pick1, rows, preferred_element_type=jnp.float32)
        return out0 * weight0 + out1 * weight1

    def blocks_back(j):
        with jax.named_scope("wait_rb"):
            arrived(ret_b.at[:, pl.ds(1, PEERS - 1)], r_rb)
        for k in range(1, 4):
            y_out[k - 1] = weighted(picks(k), ret_b[k].reshape(PEERS * CAP, RB)).astype(jnp.bfloat16)
            put(y_out.at[k - 1], y_in.at[k - 1], send.at[9], r_y, along(4 - k))

    steps = {
        "gath": blocks_b,
        "sa": send_a,
        "sb": send_b,
        "cnt": send_counts,
        "wts": weights_in,
        "own": own,
        "fwd": forward,
        "ready": ready,
        "up": project_up,
        "down": project_down,
        "give": give_back,
        "add": add_on,
        "fin": finish,
        "blk": blocks_back,
    }
    for entry in SCHEDULE:
        with jax.named_scope(entry):
            steps[entry[:-1]](int(entry[-1]))

    with jax.named_scope("load"):
        arrived(cnt_in.at[pl.ds(1, PEERS - 1)], r_cnt)
        cnt_in[0] = cnt_out[...]
        load[...] = jnp.sum(cnt_in[...], axis=0)[:, :32]

    with jax.named_scope("own_rows"):
        mine_at = picks(0)
        own_b = weighted(mine_at, ret_b[0].reshape(PEERS * CAP, RB))
        with jax.named_scope("wait_ra"):
            arrived(ret_a.at[pl.ds(1, PEERS - 1)], r_ra)
        own_a = weighted(mine_at, ret_a[...].reshape(PEERS * CAP, RA))
    with jax.named_scope("mix"):
        mixed[:, :RA] = (frames[:, :RA].astype(jnp.float32) + own_a).astype(jnp.bfloat16)
        arrived(y_in, r_y)
        for k in range(1, 4):
            own_b = own_b + y_in[k - 1].astype(jnp.float32)
        mixed[:, RA:] = (frames[:, RA:].astype(jnp.float32) + own_b).astype(jnp.bfloat16)

    with jax.named_scope("sent"):
        rest = pl.ds(1, PEERS - 1)
        three = pl.ds(0, 3)
        arrived(info.at[pl.ds(1, 3)], send.at[0])
        arrived(norm_b.at[pl.ds(1, 3)], send.at[1])
        arrived(slots_a.at[rest], send.at[2])
        arrived(slots_b.at[:, rest], send.at[3])
        arrived(cnt_in.at[rest], send.at[4])
        arrived(x_in.at[three, :, :, wide], send.at[5])
        arrived(part.at[three, :, :, wide_back], send.at[6])
        arrived(ret_b.at[:, rest], send.at[7])
        arrived(e_out.at[rest], send.at[8])
        arrived(y_out, send.at[9])


def finish_kernel(mixed_in, load_in, mixed, load, sems):
    copies = [
        pltpu.make_async_copy(mixed_in, mixed, sems.at[0]),
        pltpu.make_async_copy(load_in, load, sems.at[1]),
    ]
    for copy in copies:
        copy.start()
    for copy in copies:
        copy.wait()


def per_device(frames, gain, nbias, routes, codes, limits, up_w, up_b, down_w, down_b):
    vmem = pl.BlockSpec(memory_space=pltpu.VMEM)
    hbm = pl.BlockSpec(memory_space=pltpu.HBM)
    bf16, f32, i32 = jnp.bfloat16, jnp.float32, jnp.int32
    dma = pltpu.SemaphoreType.DMA
    mixed, load = pl.pallas_call(
        kernel,
        out_shape=(
            jax.ShapeDtypeStruct((FRAMES, D), bf16),
            jax.ShapeDtypeStruct((1, 32), i32),
        ),
        in_specs=[hbm] * 10,
        out_specs=(vmem, vmem),
        scratch_shapes=[
            pltpu.VMEM((FRAMES, D), bf16),
            pltpu.VMEM((3, 1, D), f32),
            pltpu.VMEM((2, 2, FRAMES), i32),
            pltpu.SMEM((32,), i32),
            pltpu.VMEM((8, D), f32),
            pltpu.VMEM((2, D, D), bf16),
            pltpu.VMEM((PEERS, CAP, CA), bf16),
            pltpu.VMEM((4, FRAMES, CB), bf16),
            pltpu.VMEM((4, PEERS, CAP, CB), bf16),
            pltpu.VMEM((4, PEERS, CAP, D), bf16),
            pltpu.VMEM((4 * max(SIZES) * CAP, D), bf16),
            pltpu.VMEM((4, PEERS, CAP, D), bf16),
            pltpu.VMEM((2, PEERS // 2, CAP, RA), bf16),
            pltpu.VMEM((2, PEERS, CAP, RA), bf16),
            pltpu.VMEM((PEERS, CAP, RA), bf16),
            pltpu.VMEM((PEERS, CAP, RA), bf16),
            pltpu.VMEM((4, PEERS, CAP, RB), bf16),
            pltpu.VMEM((3, FRAMES, RB), bf16),
            pltpu.VMEM((3, FRAMES, RB), bf16),
            pltpu.VMEM((4, 8, FRAMES), i32),
            pltpu.VMEM((1, FRAMES), i32),
            pltpu.VMEM((PEERS, 1, FRAMES), i32),
            pltpu.VMEM((1, D), f32),
            dma((6,)),
            dma((10,)),
            dma((CHUNKS,)),
            dma((CHUNKS,)),
            dma,
            dma((3,)),
            dma((CHUNKS,)),
            dma((CHUNKS,)),
            dma((CHUNKS,)),
            dma((CHUNKS,)),
            dma((CHUNKS,)),
            dma,
            dma,
            dma,
            dma,
        ],
        compiler_params=pltpu.CompilerParams(
            collective_id=0, has_side_effects=True, vmem_limit_bytes=30 << 20
        ),
        name="moe",
    )(
        *[
            pltpu.with_memory_space_constraint(value, pltpu.HBM)
            for value in (
                frames,
                gain.reshape(1, D),
                nbias.reshape(1, D),
                routes.T,
                codes.T,
                limits,
                up_w,
                up_b,
                down_w,
                down_b,
            )
        ],
    )
    mixed, load = pl.pallas_call(
        finish_kernel,
        out_shape=(
            jax.ShapeDtypeStruct((FRAMES, D), bf16),
            jax.ShapeDtypeStruct((1, 32), i32),
        ),
        in_specs=[vmem, vmem],
        out_specs=(hbm, hbm),
        scratch_shapes=[dma((2,))],
        compiler_params=pltpu.CompilerParams(vmem_limit_bytes=1 << 20),
        name="store",
    )(mixed, load)
    return mixed, load.reshape(32)


def solution(mesh):
    both = ("dp", "expert")
    in_specs = (
        P(both, None),
        P(),
        P(),
        P(both, None),
        P(both, None),
        P(),
        P(both, None, None),
        P(both, None),
        P(both, None, None),
        P(),
    )
    out_specs = (P(both, None), P())
    return jax.shard_map(
        per_device, mesh=mesh, in_specs=in_specs, out_specs=out_specs, check_vma=False
    )
```

```python
import jax
import jax.numpy as jnp
from jax import lax
from jax.experimental import pallas as pl
from jax.experimental.pallas import tpu as pltpu
from jax.sharding import PartitionSpec as P

MESH = pl.DeviceIdType.MESH
EPS = 1e-05
D = 1024
FRAMES = 128
CAP = 16
PEERS = 32
CB = 384
CA = D - CB
RB = 384
RA = D - RB
SIZES = [8, 8, 8, 8]
CHUNKS = len(SIZES)
LOAD_SEM = [0, 0, 1, 2, 3, 3, 3, 4, 5, 5]
STARTS = [sum(SIZES[:j]) for j in range(CHUNKS + 1)]
CHUNK_OF = [j for j in range(CHUNKS) for _ in range(SIZES[j])]
TILE = 256


OFFSETS = [((n // 2) % 4, n // 8, n % 2) for n in range(PEERS)]


ORDER = [
    0, 18, 30, 14, 26, 6, 8, 2, 15, 13, 1, 27, 17, 31, 28, 10,
    21, 25, 4, 19, 23, 16, 12, 5, 20, 29, 22, 11, 7, 9, 3, 24,
]
SCHEDULE = [
    "sa0", "sa1", "sa2", "sa3", "own0", "gath0", "sb0", "sb1",
    "sb2", "sb3", "own1", "fwd0", "own2", "fwd1", "own3", "wts0",
    "ready0", "up0", "fwd2", "down0", "give0", "cnt0", "ready1", "up1",
    "fwd3", "down1", "give1", "ready2", "up2", "add0", "down2", "give2",
    "ready3", "up3", "add1", "down3", "give3", "fin0", "add2", "fin1",
    "add3", "fin2", "blk0", "fin3",
]


def kernel(
    frames_hbm,
    gain_hbm,
    nbias_hbm,
    routes_hbm,
    codes_hbm,
    limits_hbm,
    up_hbm,
    up_b_hbm,
    down_hbm,
    down_b_hbm,
    mixed,
    load,
    frames,
    vectors,
    pairs,
    limits,
    down_b,
    weights,
    slots_a,
    norm_b,
    slots_b,
    x_in,
    hid,
    part,
    t,
    g,
    e_out,
    ret_a,
    ret_b,
    y_out,
    y_in,
    info,
    cnt_out,
    cnt_in,
    brow,
    w_sem,
    send,
    r_a,
    r_b,
    r_info,
    r_nb,
    f_l,
    f_r,
    r_h,
    r_t,
    r_g,
    r_ra,
    r_rb,
    r_y,
    r_cnt,
):
    dp = lax.axis_index("dp")
    ex = lax.axis_index("expert")
    x, y = lax.rem(ex, 4), lax.div(ex, 4)
    z, c = lax.div(dp, 2), lax.rem(dp, 2)
    mine = dp * 4 + y

    zs = [lax.rem(z + k, 4) * 2 for k in range(4)]
    ys = [lax.rem(y + k, 4) * 4 + x for k in range(4)]
    cs = [c, 1 - c]

    def plane(n):
        dy, dz, dc = OFFSETS[n]
        return (zs[dz] + cs[dc], ys[dy])

    def source(n):
        dy, dz, dc = OFFSETS[n]
        return (zs[-dz] + cs[dc], ys[-dy])

    def along(k):
        return (dp, y * 4 + lax.rem(x + k, 4))

    def put(src, dst, s, r, where):
        pltpu.make_async_remote_copy(
            src, dst, s, r, device_id=where, device_id_type=MESH
        ).start()

    def arrived(ref, sem):
        pltpu.make_async_copy(ref, ref, sem).wait()

    with jax.named_scope("greet"):
        loads = [
            pltpu.make_async_copy(src, dst, w_sem.at[LOAD_SEM[i]])
            for i, (src, dst) in enumerate(
                [
                    (routes_hbm, pairs.at[0]),
                    (codes_hbm, pairs.at[1]),
                    (limits_hbm, limits),
                    (frames_hbm, frames),
                    (gain_hbm, vectors.at[0]),
                    (nbias_hbm, vectors.at[1]),
                    (up_b_hbm, vectors.at[2]),
                    (down_b_hbm.at[pl.ds(pl.multiple_of(lax.div(mine, 8) * 8, 8), 8)], down_b),
                    (up_hbm.at[0], weights.at[0]),
                    (down_hbm.at[0], weights.at[1]),
                ]
            )
        ]
        for copy in loads:
            copy.start()
        barrier = pltpu.get_barrier_semaphore()
        for n in range(1, PEERS):
            pl.semaphore_signal(barrier, inc=1, device_id=plane(n), device_id_type=MESH)
        for k in range(1, 4):
            pl.semaphore_signal(barrier, inc=1, device_id=along(k), device_id_type=MESH)
        arrived(pairs, w_sem.at[0])
        loads[2].wait()

    with jax.named_scope("route"):
        chosen = pairs[0]
        ids = lax.broadcasted_iota(jnp.int32, (FRAMES, FRAMES), 0)
        cols = lax.broadcasted_iota(jnp.int32, (FRAMES, FRAMES), 1)
        hit0 = (ids == chosen[0:1, :]).astype(jnp.float32)
        hit1 = (ids == chosen[1:2, :]).astype(jnp.float32)
        before = (ids < cols).astype(jnp.bfloat16)
        earlier = jnp.dot(
            (hit0 + hit1).astype(jnp.bfloat16), before, preferred_element_type=jnp.float32
        )
        rank = jnp.concatenate(
            [
                jnp.sum(earlier * hit0, axis=0, keepdims=True),
                jnp.sum(earlier * hit1, axis=0, keepdims=True),
            ],
            axis=0,
        ).astype(jnp.int32)
        bound = jnp.zeros((2, FRAMES), jnp.int32)
        for e in range(32):
            bound = jnp.where(chosen == e, limits[e], bound)
        kept = rank < bound
        dz = (lax.shift_right_logical(chosen, 3) - z + 4) & 3
        dc = ((lax.shift_right_logical(chosen, 2) & 1) - c + 2) & 1
        dy = ((chosen & 3) - y + 4) & 3
        spot = jnp.where(kept, ((dz * 4 + dy) * 2 + dc) * CAP + rank, -1)
        keptf = kept.astype(jnp.float32)
        taken = (hit0 * keptf[0:1, :] + hit1 * keptf[1:2, :]).astype(jnp.bfloat16)
        counts = lax.dot_general(
            jnp.ones((8, FRAMES), jnp.bfloat16),
            taken,
            (((1,), (1,)), ((), ())),
            preferred_element_type=jnp.float32,
        ).astype(jnp.int32)
        info[0, 0:2, :] = spot
        info[0, 2:4, :] = pairs[1]
        info[0, 4:8, :] = counts[0:4, :]

    with jax.named_scope("norm"):
        loads[3].wait()
        arrived(vectors, w_sem.at[3])
        values = frames[...].astype(jnp.float32)
        center = jnp.mean(values, axis=-1, keepdims=True)
        shifted = values - center
        spread = jnp.mean(shifted * shifted, axis=-1, keepdims=True)
        normed = (shifted * lax.rsqrt(spread + EPS) * vectors[0] + vectors[1]).astype(jnp.bfloat16)
        norm_b[0] = normed[:, CA:]

    slot_ids = lax.broadcasted_iota(jnp.int32, (PEERS * CAP, FRAMES), 0)

    def gathered(k, rows):
        spots = info[k]
        pick = (slot_ids == spots[0:1, :]) | (slot_ids == spots[1:2, :])
        return (
            jnp.dot(
                pick.astype(jnp.float32).astype(jnp.bfloat16),
                rows,
                preferred_element_type=jnp.float32,
            )
            .astype(jnp.bfloat16)
            .reshape(PEERS, CAP, rows.shape[1])
        )

    with jax.named_scope("gather"):
        slots_a[...] = gathered(0, normed[:, :CA])
        loads[7].wait()
        row = down_b[pl.ds(lax.rem(mine, 8), 1), :]
        lane = lax.broadcasted_iota(jnp.int32, (1, D), 1)
        brow[...] = jnp.where(lane >= RA, row * 0.25, 0.0)
        x_in[0, 0, :, :CA] = slots_a[0]

    with jax.named_scope("met"):
        pl.semaphore_wait(barrier, PEERS - 1 + 3)
    with jax.named_scope("send_a"):
        for k in range(1, 4):
            put(info.at[0], info.at[k], send.at[0], r_info, along(k))
            put(norm_b.at[0], norm_b.at[k], send.at[1], r_nb.at[k - 1], along(k))

    def chunk(j):
        return pl.ds(STARTS[j], SIZES[j])

    def first(j):
        return pl.ds(STARTS[j], SIZES[j] // 2)

    def second(j):
        return pl.ds(STARTS[j] + SIZES[j] // 2, SIZES[j] // 2)

    def halves(j):
        return pl.ds(STARTS[j] // 2, SIZES[j] // 2)

    def remote(j):
        begin = max(STARTS[j], 1)
        return pl.ds(begin, STARTS[j + 1] - begin)

    wide = pl.ds(0, CA)
    narrow = pl.ds(CA, CB)
    wide_back = pl.ds(0, RA)
    narrow_back = pl.ds(RA, RB)

    def own(j):
        arrived(x_in.at[0, remote(j), :, wide], r_a.at[j])
        put(
            x_in.at[0, chunk(j), :, wide],
            x_in.at[1, chunk(j), :, wide],
            send.at[5],
            f_l.at[j],
            along(1),
        )
        put(
            x_in.at[0, chunk(j), :, wide],
            x_in.at[3, chunk(j), :, wide],
            send.at[5],
            f_r.at[j],
            along(3),
        )

    def forward(j):
        arrived(x_in.at[1, chunk(j), :, wide], f_l.at[j])
        put(
            x_in.at[1, first(j), :, wide],
            x_in.at[2, first(j), :, wide],
            send.at[5],
            r_h.at[j],
            along(1),
        )
        arrived(x_in.at[3, chunk(j), :, wide], f_r.at[j])
        put(
            x_in.at[3, second(j), :, wide],
            x_in.at[2, second(j), :, wide],
            send.at[5],
            r_h.at[j],
            along(3),
        )

    def ready(j):
        arrived(x_in.at[:, remote(j), :, narrow], r_b.at[j])
        arrived(x_in.at[2, chunk(j), :, wide], r_h.at[j])

    def project_up(j):
        def step(t, carry):
            lanes = pl.ds(pl.multiple_of(t * TILE, TILE), TILE)
            rows = x_in[:, STARTS[j] : STARTS[j + 1]].reshape(4 * SIZES[j] * CAP, D)
            pre = jnp.dot(rows, weights[0, :, lanes], preferred_element_type=jnp.float32)
            pre = pre + vectors[2, :, lanes]
            act = 0.5 * pre * (1.0 + lax.erf(pre * 0.7071067811865476))
            hid[: 4 * SIZES[j] * CAP, lanes] = act.astype(jnp.bfloat16)
            return carry

        lax.fori_loop(0, D // TILE, step, 0)

    def project_down(j):
        def step(t, carry):
            lanes = pl.ds(pl.multiple_of(t * TILE, TILE), TILE)
            out = jnp.dot(hid[: 4 * SIZES[j] * CAP], weights[1, :, lanes], preferred_element_type=jnp.float32)
            out = out + brow[:, lanes]
            part[:, STARTS[j] : STARTS[j + 1], :, lanes] = out.astype(jnp.bfloat16).reshape(
                4, SIZES[j], CAP, TILE
            )
            return carry

        lax.fori_loop(0, D // TILE, step, 0)

    def give_back(j):
        put(part.at[2, first(j), :, wide_back], t.at[0, halves(j)], send.at[6], r_t.at[j], along(1))
        put(part.at[2, second(j), :, wide_back], t.at[1, halves(j)], send.at[6], r_t.at[j], along(3))
        put(part.at[3, second(j), :, wide_back], g.at[0, second(j)], send.at[6], r_g.at[j], along(1))
        put(part.at[1, first(j), :, wide_back], g.at[1, first(j)], send.at[6], r_g.at[j], along(3))
        for p in range(STARTS[j], STARTS[j + 1]):
            if p:
                put(
                    part.at[:, p, :, narrow_back],
                    ret_b.at[:, ORDER[p]],
                    send.at[7],
                    r_rb,
                    source(ORDER[p]),
                )
            else:
                ret_b[:, 0] = part[:, 0, :, RA:]

    def add_on(j):
        arrived(t.at[:, halves(j)], r_t.at[j])
        spots = slice(STARTS[j], STARTS[j] + SIZES[j] // 2)
        part[3, spots, :, :RA] = (
            part[3, spots, :, :RA].astype(jnp.float32) + t[0, STARTS[j] // 2 : STARTS[j + 1] // 2].astype(jnp.float32)
        ).astype(jnp.bfloat16)
        put(part.at[3, first(j), :, wide_back], g.at[0, first(j)], send.at[6], r_g.at[j], along(1))
        spots = slice(STARTS[j] + SIZES[j] // 2, STARTS[j + 1])
        part[1, spots, :, :RA] = (
            part[1, spots, :, :RA].astype(jnp.float32) + t[1, STARTS[j] // 2 : STARTS[j + 1] // 2].astype(jnp.float32)
        ).astype(jnp.bfloat16)
        put(part.at[1, second(j), :, wide_back], g.at[1, second(j)], send.at[6], r_g.at[j], along(3))

    def finish(j):
        arrived(g.at[:, chunk(j)], r_g.at[j])
        spots = slice(STARTS[j], STARTS[j + 1])
        bias = row[:, :RA].reshape(1, 1, RA)
        e_out[spots] = (
            part[0, spots, :, :RA].astype(jnp.float32)
            + g[0, spots].astype(jnp.float32)
            + g[1, spots].astype(jnp.float32)
            + bias
        ).astype(jnp.bfloat16)
        for p in range(STARTS[j], STARTS[j + 1]):
            if p:
                put(e_out.at[p], ret_a.at[ORDER[p]], send.at[8], r_ra, source(ORDER[p]))
            else:
                ret_a[0] = e_out[0]

    def blocks_b(j):
        slots_b[0] = gathered(0, normed[:, CA:])
        total = info[0, 4:5, :]
        arrived(info.at[pl.ds(1, 3)], r_info)
        for k in range(1, 4):
            arrived(norm_b.at[k], r_nb.at[k - 1])
            slots_b[k] = gathered(k, norm_b[k])
            total = total + info[k, 4:5, :]
        cnt_out[...] = total
        x_in[:, 0, :, CA:] = slots_b[:, 0]

    def send_a(j):
        for p in range(max(STARTS[j], 1), STARTS[j + 1]):
            n = ORDER[p]
            put(
                slots_a.at[n],
                x_in.at[0, p, :, pl.ds(0, CA)],
                send.at[2],
                r_a.at[j],
                plane(n),
            )

    def send_b(j):
        for p in range(max(STARTS[j], 1), STARTS[j + 1]):
            n = ORDER[p]
            put(
                slots_b.at[:, n],
                x_in.at[:, p, :, pl.ds(CA, CB)],
                send.at[3],
                r_b.at[j],
                plane(n),
            )

    def send_counts(j):
        for n in range(1, PEERS):
            put(cnt_out, cnt_in.at[n], send.at[4], r_cnt, plane(n))

    def weights_in(j):
        arrived(weights, w_sem.at[5])

    slot_cols = lax.broadcasted_iota(jnp.int32, (FRAMES, PEERS * CAP), 1)

    def picks(k):
        table = jnp.concatenate([info[k], jnp.zeros((FRAMES - 8, FRAMES), jnp.int32)], axis=0)
        turned = jnp.transpose(table.astype(jnp.float32))
        code0, code1 = turned[:, 2:3], turned[:, 3:4]
        weight0 = code0 / (code0 + code1)
        weight1 = code1 / (code0 + code1)
        spots = turned.astype(jnp.int32)
        pick0 = (slot_cols == spots[:, 0:1]).astype(jnp.float32).astype(jnp.bfloat16)
        pick1 = (slot_cols == spots[:, 1:2]).astype(jnp.float32).astype(jnp.bfloat16)
        return pick0, pick1, weight0, weight1

    def weighted(found, rows):
        pick0, pick1, weight0, weight1 = found
        out0 = jnp.dot(pick0, rows, preferred_element_type=jnp.float32)
        out1 = jnp.dot(pick1, rows, preferred_element_type=jnp.float32)
        return out0 * weight0 + out1 * weight1

    def blocks_back(j):
        with jax.named_scope("wait_rb"):
            arrived(ret_b.at[:, pl.ds(1, PEERS - 1)], r_rb)
        for k in range(1, 4):
            y_out[k - 1] = weighted(picks(k), ret_b[k].reshape(PEERS * CAP, RB)).astype(jnp.bfloat16)
            put(y_out.at[k - 1], y_in.at[k - 1], send.at[9], r_y, along(4 - k))

    steps = {
        "gath": blocks_b,
        "sa": send_a,
        "sb": send_b,
        "cnt": send_counts,
        "wts": weights_in,
        "own": own,
        "fwd": forward,
        "ready": ready,
        "up": project_up,
        "down": project_down,
        "give": give_back,
        "add": add_on,
        "fin": finish,
        "blk": blocks_back,
    }
    for entry in SCHEDULE:
        with jax.named_scope(entry):
            steps[entry[:-1]](int(entry[-1]))

    with jax.named_scope("load"):
        arrived(cnt_in.at[pl.ds(1, PEERS - 1)], r_cnt)
        cnt_in[0] = cnt_out[...]
        load[...] = jnp.sum(cnt_in[...], axis=0)[:, :32]

    with jax.named_scope("own_rows"):
        mine_at = picks(0)
        own_b = weighted(mine_at, ret_b[0].reshape(PEERS * CAP, RB))
        with jax.named_scope("wait_ra"):
            arrived(ret_a.at[pl.ds(1, PEERS - 1)], r_ra)
        own_a = weighted(mine_at, ret_a[...].reshape(PEERS * CAP, RA))
    with jax.named_scope("mix"):
        mixed[:, :RA] = (frames[:, :RA].astype(jnp.float32) + own_a).astype(jnp.bfloat16)
        arrived(y_in, r_y)
        for k in range(1, 4):
            own_b = own_b + y_in[k - 1].astype(jnp.float32)
        mixed[:, RA:] = (frames[:, RA:].astype(jnp.float32) + own_b).astype(jnp.bfloat16)

    with jax.named_scope("sent"):
        rest = pl.ds(1, PEERS - 1)
        three = pl.ds(0, 3)
        arrived(info.at[pl.ds(1, 3)], send.at[0])
        arrived(norm_b.at[pl.ds(1, 3)], send.at[1])
        arrived(slots_a.at[rest], send.at[2])
        arrived(slots_b.at[:, rest], send.at[3])
        arrived(cnt_in.at[rest], send.at[4])
        arrived(x_in.at[three, :, :, wide], send.at[5])
        arrived(part.at[three, :, :, wide_back], send.at[6])
        arrived(ret_b.at[:, rest], send.at[7])
        arrived(e_out.at[rest], send.at[8])
        arrived(y_out, send.at[9])


def finish_kernel(mixed_in, load_in, mixed, load, sems):
    copies = [
        pltpu.make_async_copy(mixed_in, mixed, sems.at[0]),
        pltpu.make_async_copy(load_in, load, sems.at[1]),
    ]
    for copy in copies:
        copy.start()
    for copy in copies:
        copy.wait()


def per_device(frames, gain, nbias, routes, codes, limits, up_w, up_b, down_w, down_b):
    vmem = pl.BlockSpec(memory_space=pltpu.VMEM)
    hbm = pl.BlockSpec(memory_space=pltpu.HBM)
    bf16, f32, i32 = jnp.bfloat16, jnp.float32, jnp.int32
    dma = pltpu.SemaphoreType.DMA
    mixed, load = pl.pallas_call(
        kernel,
        out_shape=(
            jax.ShapeDtypeStruct((FRAMES, D), bf16),
            jax.ShapeDtypeStruct((1, 32), i32),
        ),
        in_specs=[hbm] * 10,
        out_specs=(vmem, vmem),
        scratch_shapes=[
            pltpu.VMEM((FRAMES, D), bf16),
            pltpu.VMEM((3, 1, D), f32),
            pltpu.VMEM((2, 2, FRAMES), i32),
            pltpu.SMEM((32,), i32),
            pltpu.VMEM((8, D), f32),
            pltpu.VMEM((2, D, D), bf16),
            pltpu.VMEM((PEERS, CAP, CA), bf16),
            pltpu.VMEM((4, FRAMES, CB), bf16),
            pltpu.VMEM((4, PEERS, CAP, CB), bf16),
            pltpu.VMEM((4, PEERS, CAP, D), bf16),
            pltpu.VMEM((4 * max(SIZES) * CAP, D), bf16),
            pltpu.VMEM((4, PEERS, CAP, D), bf16),
            pltpu.VMEM((2, PEERS // 2, CAP, RA), bf16),
            pltpu.VMEM((2, PEERS, CAP, RA), bf16),
            pltpu.VMEM((PEERS, CAP, RA), bf16),
            pltpu.VMEM((PEERS, CAP, RA), bf16),
            pltpu.VMEM((4, PEERS, CAP, RB), bf16),
            pltpu.VMEM((3, FRAMES, RB), bf16),
            pltpu.VMEM((3, FRAMES, RB), bf16),
            pltpu.VMEM((4, 8, FRAMES), i32),
            pltpu.VMEM((1, FRAMES), i32),
            pltpu.VMEM((PEERS, 1, FRAMES), i32),
            pltpu.VMEM((1, D), f32),
            dma((6,)),
            dma((10,)),
            dma((CHUNKS,)),
            dma((CHUNKS,)),
            dma,
            dma((3,)),
            dma((CHUNKS,)),
            dma((CHUNKS,)),
            dma((CHUNKS,)),
            dma((CHUNKS,)),
            dma((CHUNKS,)),
            dma,
            dma,
            dma,
            dma,
        ],
        compiler_params=pltpu.CompilerParams(
            collective_id=0, has_side_effects=True, vmem_limit_bytes=30 << 20
        ),
        name="moe",
    )(
        *[
            pltpu.with_memory_space_constraint(value, pltpu.HBM)
            for value in (
                frames,
                gain.reshape(1, D),
                nbias.reshape(1, D),
                routes.T,
                codes.T,
                limits,
                up_w,
                up_b,
                down_w,
                down_b,
            )
        ],
    )
    mixed, load = pl.pallas_call(
        finish_kernel,
        out_shape=(
            jax.ShapeDtypeStruct((FRAMES, D), bf16),
            jax.ShapeDtypeStruct((1, 32), i32),
        ),
        in_specs=[vmem, vmem],
        out_specs=(hbm, hbm),
        scratch_shapes=[dma((2,))],
        compiler_params=pltpu.CompilerParams(vmem_limit_bytes=1 << 20),
        name="store",
    )(mixed, load)
    return mixed, load.reshape(32)


def solution(mesh):
    both = ("dp", "expert")
    in_specs = (
        P(both, None),
        P(),
        P(),
        P(both, None),
        P(both, None),
        P(),
        P(both, None, None),
        P(both, None),
        P(both, None, None),
        P(),
    )
    out_specs = (P(both, None), P())
    return jax.shard_map(
        per_device, mesh=mesh, in_specs=in_specs, out_specs=out_specs, check_vma=False
    )
```
